128 devices in a mesh: dp: 16 (over y, x), expert: 8 (over z, core).
Axes of the slice: x: 4, y: 4, z: 4, core: 2. Of those that a mesh axis runs over, the one named last changes fastest.
Arguments:
- tokens: bfloat16 [16384, 4096], P(('dp', 'expert')), may hold values from -6 to 6
- probs: bfloat16 [16384, 1], P(('dp', 'expert')), may hold values from 0.19921875 to 1
- routes: int32 [16384, 1], P(('dp', 'expert')), may hold values from 0 to 7; in each aligned block of 128 rows (0 to 127, 128 to 255, ...) at most 17 rows name the same one
- w_gate: bfloat16 [8, 4096, 1024], P('expert', 'dp'), may hold values from -0.09375 to 0.09375
- w_up: bfloat16 [8, 4096, 1024], P('expert', 'dp'), may hold values from -0.09375 to 0.09375
- w_down: bfloat16 [8, 1024, 4096], P('expert', None, 'dp'), may hold values from -0.1875 to 0.1875
- cotangent: bfloat16 [16384, 4096], P(('dp', 'expert')), may hold values from -6 to 6
Outputs:
- mixed: bfloat16 [16384, 4096], P(('dp', 'expert'))
- input_grad: bfloat16 [16384, 4096], P(('dp', 'expert'))
- grad_gate: bfloat16 [8, 4096, 1024], P('expert', 'dp')
- grad_up: bfloat16 [8, 4096, 1024], P('expert', 'dp')
- grad_down: bfloat16 [8, 1024, 4096], P('expert', None, 'dp')
The draws below stay inside these ranges and needn't reach their ends.
Inputs may be any that keep to these rules, and one draw needn't show every extreme that they name: `routes`: each row names exactly one expert. Among the 128 rows of one device (aligned blocks), no expert is named more than 17 times, a bound that some block reaches.
All inputs are finite; a program needn't handle non-finite values.
Results may differ from the reference program's by a relative error of at most 0.025.
Values may be sent and summed in bfloat16 or wider, within the bound.
No kernel may reach another device: no remote copies, remote signals or barrier semaphores. Data moves between devices by JAX's collectives and lax.ppermute only.
A program may use at most 128 MiB of HBM per device.

```python
import math
import jax
import jax.numpy as jnp
import numpy as np
from jax import lax

D = 4096
FF = 1024
TOP = 1
TOK_DEV = 128
EXPERTS = 8
CAP = 17
TOKENS = 16384
N_DP = 16
N_EXPERT = 8


def block_levels(stream_key, extent, pieces, least, largest):
    gain = 1.0
    for axis_at, shards_of in pieces:
        heights = jax.random.uniform(jax.random.fold_in(jax.random.fold_in(stream_key, 6), axis_at), (shards_of,), jnp.float32, least / len(pieces), largest / len(pieces))
        gain = gain * jnp.repeat(jnp.exp(heights), extent[axis_at] // shards_of).reshape((-1,) + (1,) * (len(extent) - 1 - axis_at))
    return gain


def shared_out(own_key, own, number, rows, count, top, most, lean):
    ranking = jax.random.permutation(own_key, count)
    packed, usual = shares(count, rows * top, most, lean, True), shares(count, rows * top, most, lean, False)
    places = jnp.arange(count)

    def named(sizes, rotation):
        used = int((sizes > 0).sum())
        fixed = max(1, used // 4)
        shifted = fixed + (places - fixed + rotation * (used - fixed)) % max(1, count - fixed)
        return jnp.zeros((count,), jnp.int32).at[ranking[jnp.where(places < fixed, places, shifted)]].set(jnp.asarray(sizes, jnp.int32))

    sizes = jnp.where(number % 4 == 0, named(packed, number // 4), named(usual, number - number // 4 - 1))
    mixed = jax.random.permutation(jax.random.fold_in(own, 3), count)
    giver, receiver = mixed[0:count // 2 * 2:2], mixed[1:count // 2 * 2:2]
    room = jnp.minimum(sizes[giver] - 1, most - sizes[receiver]) // 2
    room = jnp.where((giver == ranking[0]) | (receiver == ranking[0]) | (sizes[receiver] == 0), 0, jnp.maximum(room, 0))
    shifted = jax.random.randint(jax.random.fold_in(own, 4), (count // 2,), 0, 1 << 20) % (room + 1)
    sizes = sizes.at[giver].add(-shifted).at[receiver].add(shifted)
    labels = jnp.searchsorted(jnp.cumsum(sizes), jnp.arange(rows * top), side="right").astype(jnp.int32)
    listing = labels.reshape(top, rows).T
    listing = listing[jax.random.permutation(jax.random.fold_in(own, 1), rows)]
    rotation = jax.random.randint(jax.random.fold_in(own, 2), (rows, 1), 0, top)
    return jnp.take_along_axis(listing, (jnp.arange(top)[None, :] + rotation) % top, axis=1)


def shares(number_of, total, reach, lean, full):
    loads = [(1 << 20) // math.isqrt(grade ** lean) + 1 for grade in range(1, number_of + 1)]
    largest = reach if full else min(reach, max(-(-total // number_of), total * loads[0] // sum(loads)))
    least = 1 if total - largest >= number_of - 1 else 0
    holding, rest = [largest] + [least] * (number_of - 1), total - largest - least * (number_of - 1)
    while rest > 0:
        free = [i for i in range(1, number_of) if holding[i] < largest] or [i for i in range(1, number_of) if holding[i] < reach]
        whole, left = sum([loads[i] for i in free]), rest
        for i in free:
            extra = min(reach - holding[i], max(1, left * loads[i] // whole), rest)
            holding[i] = holding[i] + extra
            rest = rest - extra
    return np.array(holding)


def centred(rng, shape, scale, bound, shards=(), held_as=jnp.bfloat16):
    loudness = block_levels(rng, shape, shards, -0.22, 0.18) if shards else 1.0
    values = jax.random.normal(rng, shape, jnp.float32) * scale * loudness
    return jnp.minimum(jnp.maximum(values, -bound), bound).astype(held_as)


def setup_inputs(seed: int = 0) -> dict:
    seeds = jax.random.split(jax.random.key(seed), 8)
    tokens = centred(seeds[0], (TOKENS, D), 1.0, 6.0, ((0, 128),))
    probs = jnp.clip(jnp.exp(math.log(1.0) - 1.6133518 * jax.random.uniform(seeds[1], (TOKENS, TOP), jnp.float32) ** block_levels(seeds[1], (TOKENS, TOP), ((0, 128),), -0.2, 0.2)), 0.19921875, 1.0).astype(jnp.bfloat16)
    routes_keys = jax.random.split(jax.random.fold_in(seeds[2], 1), TOKENS // TOK_DEV)
    routes_turns = jax.random.permutation(jax.random.fold_in(seeds[2], 3), TOKENS // TOK_DEV)
    routes = jax.vmap(lambda own, number: shared_out(jax.random.fold_in(seeds[2], 2), own, number, TOK_DEV, EXPERTS, TOP, CAP, 2))(routes_keys, routes_turns).reshape((TOKENS, TOP))
    w_gate = centred(seeds[3], (EXPERTS, D, FF), D ** -0.5, 0.09375, ((0, 8), (1, 16)))
    w_up = centred(seeds[4], (EXPERTS, D, FF), D ** -0.5, 0.09375, ((0, 8), (1, 16)))
    w_down = centred(seeds[5], (EXPERTS, FF, D), FF ** -0.5, 0.1875, ((0, 8), (2, 16)))
    cotangent = centred(seeds[6], (TOKENS, D), 1.0, 6.0, ((0, 128),))
    return dict(tokens=tokens, probs=probs, routes=routes, w_gate=w_gate, w_up=w_up, w_down=w_down, cotangent=cotangent)


def split_sum(left, right):
    parts = jnp.einsum("rnk,nkf->nrf", left.astype(jnp.float32), right.astype(jnp.float32),
                       precision=lax.Precision.HIGHEST)
    rounded = lax.optimization_barrier(parts.astype(jnp.bfloat16))
    return jnp.sum(rounded.astype(jnp.float32), axis=0)


def reference(tokens, probs, routes, w_gate, w_up, w_down, cotangent):
    flat_route = routes.reshape(-1)
    flat_prob = probs.reshape(-1)
    most = N_DP * N_EXPERT * CAP
    slices = D // N_DP

    def one_expert(carry, expert):
        mixed_sum, input_sum = carry
        hit = flat_route == expert
        pick = jnp.nonzero(hit, size=most, fill_value=0)[0].astype(jnp.int32)
        valid = jnp.arange(most, dtype=jnp.int32) < jnp.sum(hit.astype(jnp.int32))
        keep = valid.astype(jnp.float32)
        owner = (pick // TOP).astype(jnp.int32)
        rows = tokens[owner] * valid[:, None].astype(jnp.bfloat16)
        weight = flat_prob[pick].astype(jnp.float32) * keep
        gate_w = lax.dynamic_index_in_dim(w_gate, expert, 0, keepdims=False)
        up_w = lax.dynamic_index_in_dim(w_up, expert, 0, keepdims=False)
        down_w = lax.dynamic_index_in_dim(w_down, expert, 0, keepdims=False)
        split_rows = rows.reshape(most, N_DP, slices)
        gate_pre = split_sum(split_rows, gate_w.reshape(N_DP, slices, FF))
        up_value = split_sum(split_rows, up_w.reshape(N_DP, slices, FF))
        sig = jax.nn.sigmoid(gate_pre)
        act = (gate_pre * sig * up_value).astype(jnp.bfloat16)
        result = jnp.dot(act, down_w, preferred_element_type=jnp.float32).astype(jnp.bfloat16)
        mixed_sum = mixed_sum.at[owner].add(result.astype(jnp.float32) * weight[:, None])
        dout = (cotangent[owner].astype(jnp.float32) * weight[:, None]).astype(jnp.bfloat16)
        grad_down = jnp.dot(act.T, dout, preferred_element_type=jnp.float32).astype(jnp.bfloat16)
        down_split = jnp.transpose(down_w.reshape(FF, N_DP, slices), (1, 2, 0))
        dact = split_sum(dout.reshape(most, N_DP, slices), down_split)
        dgate = (dact * up_value * sig * (1.0 + gate_pre * (1.0 - sig))).astype(jnp.bfloat16)
        dup = (dact * gate_pre * sig).astype(jnp.bfloat16)
        grad_gate = jnp.dot(rows.T, dgate, preferred_element_type=jnp.float32).astype(jnp.bfloat16)
        grad_up = jnp.dot(rows.T, dup, preferred_element_type=jnp.float32).astype(jnp.bfloat16)
        slot_grad = (jnp.dot(dgate, gate_w.T, preferred_element_type=jnp.float32)
                     + jnp.dot(dup, up_w.T, preferred_element_type=jnp.float32)).astype(jnp.bfloat16)
        input_sum = input_sum.at[owner].add(slot_grad.astype(jnp.float32) * keep[:, None])
        return (mixed_sum, input_sum), (grad_gate, grad_up, grad_down)

    start = (jnp.zeros((TOKENS, D), jnp.float32), jnp.zeros((TOKENS, D), jnp.float32))
    (mixed_sum, input_sum), grads = lax.scan(one_expert, start, jnp.arange(EXPERTS, dtype=jnp.int32))
    return (mixed_sum.astype(jnp.bfloat16), input_sum.astype(jnp.bfloat16), grads[0], grads[1], grads[2])
```

```python
import jax
import jax.numpy as jnp
from jax import lax
from jax.experimental import pallas as pl
from jax.experimental.pallas import tpu as pltpu
from jax.sharding import Mesh
from jax.sharding import PartitionSpec as P

AXES = ("y", "x", "z", "c")
BF = jnp.bfloat16
F32 = jnp.float32
SIDE = 4
TOK = 128
BLK = 256
FF = 1024
SLOT = 36
PAIR = 2 * SLOT
SHARE = SIDE * SLOT
SENT = SIDE * PAIR
ROWS = SIDE * SHARE
WIDE = SIDE * BLK


def place(y, x, z, c):
    return ((y * SIDE + x) * SIDE + z) * 2 + c


def groups():
    n = range(SIDE)
    feature, copies, spread = [], [], []
    for k in n:
        for z in n:
            feature.append([place(k, x, z, 0) for x in n])
            feature.append([place(y, k, z, 1) for y in n])
            copies.append([place(y, k, z, 0) for y in n])
            copies.append([place(k, x, z, 1) for x in n])
        spread.append([place(k, x, z, 0) for x in n for z in n])
        spread.append([place(y, k, z, 1) for y in n for z in n])
    return feature, copies, spread


FEATURE, COPIES, SPREAD = groups()


def shifted(value, rings, step):
    pairs = [(g[(i + step) % SIDE], g[i]) for g in rings for i in range(SIDE)]
    return lax.ppermute(value, AXES, pairs)


def grouped(value, rings):
    return lax.all_to_all(value, AXES, 0, 0, axis_index_groups=rings, tiled=True)


def other_core(value):
    return lax.ppermute(value, "c", [(0, 1), (1, 0)])


def iota(shape, dim):
    return lax.broadcasted_iota(jnp.int32, shape, dim)


def dot(a, b):
    return jnp.dot(a, b, preferred_element_type=F32)


def dot_nt(a, b):
    return lax.dot_general(a, b, (((1,), (1,)), ((), ())), preferred_element_type=F32)


def dot_tn(a, b):
    return lax.dot_general(a, b, (((0,), (0,)), ((), ())), preferred_element_type=F32)


def call(body, outs, scratch=(), smem=1, n_in=0):
    specs = [pl.BlockSpec(memory_space=pltpu.SMEM)] * smem + [pl.BlockSpec(memory_space=pltpu.VMEM)] * n_in
    return pl.pallas_call(
        body,
        out_shape=outs,
        in_specs=specs,
        out_specs=jax.tree.map(lambda _: pl.BlockSpec(memory_space=pltpu.VMEM), outs),
        scratch_shapes=list(scratch),
        compiler_params=pltpu.CompilerParams(vmem_limit_bytes=56 * 2**20),
    )


def column(kind, near, group, k):
    turned = (near + k) % SIDE
    return jnp.where(kind == 0, turned * SIDE + group, group * SIDE + turned)


def row_targets(route_row, kind):
    count = route_row.shape[1]
    hits = (iota((8, count), 0) == route_row).astype(F32)
    earlier = (iota((count, count), 0) < iota((count, count), 1)).astype(BF)
    before = dot(hits.astype(BF), earlier)
    slot = jnp.sum(before * hits, axis=0, keepdims=True).astype(jnp.int32)
    return jnp.where(route_row % 2 == kind, (route_row // 2) * PAIR + slot, -PAIR)


def row_targets_t(route_col, kind):
    count = route_col.shape[0]
    hits = (iota((count, 8), 1) == route_col).astype(F32)
    earlier = (iota((count, count), 1) < iota((count, count), 0)).astype(BF)
    before = dot(earlier, hits.astype(BF))
    slot = jnp.sum(before * hits, axis=1, keepdims=True).astype(jnp.int32)
    return jnp.where(route_col % 2 == kind, (route_col // 2) * PAIR + slot, -PAIR)


def pack_body(pos, route, prob, tok_a, tok_b, cot_a, cot_b, out):
    kind, near = pos[0], pos[1]
    target = row_targets(route[...], kind)
    rows = iota((SENT, 2 * TOK), 0)
    pick_x = (rows == target).astype(BF)
    pick_y = (rows == target + SLOT).astype(BF)
    weight = prob[...]
    for d in range(SIDE):
        for k in range(SIDE):
            at = pl.ds(pl.multiple_of(column(kind, near, d, k) * BLK, BLK), BLK)
            x = jnp.concatenate([tok_a[:, at], tok_b[:, at]], axis=0)
            y = jnp.concatenate([cot_a[:, at], cot_b[:, at]], axis=0).astype(F32)
            y = (y * weight).astype(BF)
            out[d, :, k * BLK : (k + 1) * BLK] = (dot(pick_x, x) + dot(pick_y, y)).astype(BF)


def project_body(pos, got, w0, w1, w2, w3, part, x_out, y_out):
    at = pos[2]
    q, r = iota((SHARE, SENT), 0), iota((SHARE, SENT), 1)
    home = q + (q // SLOT) * SLOT
    take_x = (r == home).astype(BF)
    take_y = (r == home + SLOT).astype(BF)
    for k in range(SIDE):
        rows = got[(at + k) % SIDE]
        x_out[k * SHARE : (k + 1) * SHARE, :] = dot(take_x, rows).astype(BF)
        y_out[k * SHARE : (k + 1) * SHARE, :] = dot(take_y, rows).astype(BF)
    for t, left in enumerate((x_out, x_out, y_out)):
        for n in range(FF // BLK):
            cols = slice(n * BLK, (n + 1) * BLK)
            total = None
            for k, w in enumerate((w0, w1, w2, w3)):
                term = dot(left[:, k * BLK : (k + 1) * BLK], w[t * BLK : (t + 1) * BLK, cols])
                total = term if total is None else total + term
            total = total.astype(BF)
            for k in range(SIDE):
                part[(at + k) % SIDE, :, t * FF + n * BLK : t * FF + (n + 1) * BLK] = total[
                    k * SHARE : (k + 1) * SHARE
                ]


def activate_body(terms, out):
    for n in range(FF // BLK):
        def summed(t):
            cols = slice(t * FF + n * BLK, t * FF + (n + 1) * BLK)
            return sum(terms[s, :, cols].astype(F32) for s in range(SIDE))

        gate, upper, dact = summed(0), summed(1), summed(2)
        sig = jax.nn.sigmoid(gate)
        act = gate * sig * upper
        dgate = dact * upper * sig * (1.0 + gate * (1.0 - sig))
        dup = dact * gate * sig
        for t, v in enumerate((act, dgate, dup)):
            out[:, t * FF + n * BLK : t * FF + (n + 1) * BLK] = v.astype(BF)


def return_body(pos, a0, a1, a2, a3, w0, w1, w2, w3, back, acts, res, slot):
    at = pos[2]
    for k, a in enumerate((a0, a1, a2, a3)):
        acts[k * SHARE : (k + 1) * SHARE, :] = a[...]
    for k, w in enumerate((w0, w1, w2, w3)):
        cols = slice(k * BLK, (k + 1) * BLK)
        res[:, cols] = dot_nt(acts[:, 0:FF], w[2 * BLK : 3 * BLK, :]).astype(BF)
        grad = dot_nt(acts[:, FF : 2 * FF], w[0:BLK, :]) + dot_nt(acts[:, 2 * FF : 3 * FF], w[BLK : 2 * BLK, :])
        slot[:, cols] = grad.astype(BF)
    r, q = iota((SENT, SHARE), 0), iota((SENT, SHARE), 1)
    home = q + (q // SLOT) * SLOT
    give_m = (r == home).astype(BF)
    give_s = (r == home + SLOT).astype(BF)
    for k in range(SIDE):
        rows = slice(k * SHARE, (k + 1) * SHARE)
        back[(at + k) % SIDE] = (dot(give_m, res[rows, :]) + dot(give_s, slot[rows, :])).astype(BF)


def grads_body(x, y, acts, g0, g1, g2, g3):
    for k, g in enumerate((g0, g1, g2, g3)):
        cols = slice(k * BLK, (k + 1) * BLK)
        g[0:BLK, :] = dot_tn(x[:, cols], acts[:, FF : 2 * FF]).astype(BF)
        g[BLK : 2 * BLK, :] = dot_tn(x[:, cols], acts[:, 2 * FF : 3 * FF]).astype(BF)
        g[2 * BLK : 3 * BLK, :] = dot_tn(y[:, cols], acts[:, 0:FF]).astype(BF)


def unpack_body(pos, route_a, route_b, prob, own, oth, mixed, grad):
    kind, near, across = pos[0], pos[1], pos[2]
    mine = row_targets_t(jnp.concatenate([route_a[...], route_b[...]], axis=0), kind)[0:TOK]
    theirs = row_targets_t(jnp.concatenate([route_b[...], route_a[...]], axis=0), 1 - kind)[TOK:]
    rows = iota((TOK, SENT), 1)
    own_m, own_s = (rows == mine).astype(BF), (rows == mine + SLOT).astype(BF)
    oth_m, oth_s = (rows == theirs).astype(BF), (rows == theirs + SLOT).astype(BF)
    weight = prob[...]
    for b in range(SIDE * SIDE):
        major, minor = b // SIDE, b % SIDE
        own_d = jnp.where(kind == 0, minor, major)
        own_k = (jnp.where(kind == 0, major, minor) - near + SIDE) % SIDE
        oth_d = jnp.where(kind == 0, major, minor)
        oth_k = (jnp.where(kind == 0, minor, major) - across + SIDE) % SIDE
        o = own[own_d, :, pl.ds(pl.multiple_of(own_k * BLK, BLK), BLK)]
        t = oth[oth_d, :, pl.ds(pl.multiple_of(oth_k * BLK, BLK), BLK)]
        cols = slice(b * BLK, (b + 1) * BLK)
        mixed[:, cols] = ((dot(own_m, o) + dot(oth_m, t)) * weight).astype(BF)
        grad[:, cols] = (dot(own_s, o) + dot(oth_s, t)).astype(BF)


def total_body(g0, g1, g2, g3, gate, upper, down):
    def total(t):
        rows = slice(t * BLK, (t + 1) * BLK)
        return sum(g[rows, :].astype(F32) for g in (g0, g1, g2, g3))

    gate[...] = total(0).astype(BF)
    upper[...] = total(1).astype(BF)
    down[...] = jnp.transpose(total(2)).astype(BF)


def per_device(tokens, probs, routes, w_gate, w_up, w_down, cotangent):
    shape = lambda *dims: jax.ShapeDtypeStruct(dims, BF)
    y, x, c = lax.axis_index("y"), lax.axis_index("x"), lax.axis_index("c")
    pos = jnp.stack([c, jnp.where(c == 0, y, x), jnp.where(c == 0, x, y)]).astype(jnp.int32)
    weights = jnp.concatenate([w_gate[0], w_up[0], w_down[0].T], axis=0)
    ws = [weights] + [shifted(weights, COPIES, k) for k in (1, 2, 3)]
    prob = probs.astype(F32)
    tok_b, cot_b = other_core(tokens), other_core(cotangent)
    route_b, prob_b = other_core(routes), other_core(probs).astype(F32)
    route_row = jnp.concatenate([routes, route_b], axis=0).reshape(1, 2 * TOK)
    sent = call(pack_body, shape(SIDE, SENT, WIDE), n_in=6)(
        pos, route_row, jnp.concatenate([prob, prob_b], axis=0), tokens, tok_b, cotangent, cot_b
    )
    got = grouped(sent.reshape(SIDE * SIDE, PAIR, WIDE), SPREAD).reshape(SIDE, SENT, WIDE)
    part, rows_x, rows_y = call(
        project_body, [shape(SIDE, SHARE, 3 * FF), shape(ROWS, WIDE), shape(ROWS, WIDE)], n_in=5
    )(pos, got, *ws)
    terms = grouped(part, FEATURE)
    acts = call(activate_body, shape(SHARE, 3 * FF), smem=0, n_in=1)(terms)
    act_s = [acts] + [shifted(acts, FEATURE, k) for k in (1, 2, 3)]
    back, acts_all = call(
        return_body,
        [shape(SIDE, SENT, WIDE), shape(ROWS, 3 * FF)],
        scratch=[pltpu.VMEM((ROWS, WIDE), BF), pltpu.VMEM((ROWS, WIDE), BF)],
        n_in=8,
    )(pos, *act_s, *ws)
    own = grouped(back.reshape(SIDE * SIDE, PAIR, WIDE), SPREAD).reshape(SIDE, SENT, WIDE)
    gs = call(grads_body, [shape(3 * BLK, FF)] * SIDE, smem=0, n_in=3)(rows_x, rows_y, acts_all)
    gs = [gs[0]] + [shifted(gs[k], COPIES, -k) for k in (1, 2, 3)]
    oth = other_core(own)
    mixed, grad = call(unpack_body, [shape(TOK, SIDE * WIDE), shape(TOK, SIDE * WIDE)], n_in=5)(
        pos, routes, route_b, prob, own, oth
    )
    gate, upper, down = call(
        total_body, [shape(BLK, FF), shape(BLK, FF), shape(FF, BLK)], smem=0, n_in=4
    )(*gs)
    return mixed, grad, gate[None], upper[None], down[None]


def solution(mesh):
    finer = Mesh(mesh.devices.reshape(SIDE, SIDE, SIDE, 2), AXES)
    rows = P(AXES, None)
    wide = P(("z", "c"), ("y", "x"), None)
    tall = P(("z", "c"), None, ("y", "x"))
    return jax.shard_map(
        per_device,
        mesh=finer,
        in_specs=(rows, rows, rows, wide, wide, tall, rows),
        out_specs=(rows, rows, wide, wide, tall),
        check_vma=False,
    )
```

```python
import jax
import jax.numpy as jnp
from jax import lax
from jax.experimental import pallas as pl
from jax.experimental.pallas import tpu as pltpu
from jax.sharding import Mesh
from jax.sharding import PartitionSpec as P


AXES = ("y", "x", "z", "c")
BF = jnp.bfloat16
F32 = jnp.float32
SIDE = 4
TOK = 128
BLK = 256
FF = 1024
SLOT = 36
PAIR = 2 * SLOT
SHARE = SIDE * SLOT
SENT = SIDE * PAIR
ROWS = SIDE * SHARE
WIDE = SIDE * BLK


def place(y, x, z, c):
    return ((y * SIDE + x) * SIDE + z) * 2 + c


def groups():
    n = range(SIDE)
    feature, copies, spread = [], [], []
    for k in n:
        for z in n:
            feature.append([place(k, x, z, 0) for x in n])
            feature.append([place(y, k, z, 1) for y in n])
            copies.append([place(y, k, z, 0) for y in n])
            copies.append([place(k, x, z, 1) for x in n])
        spread.append([place(k, x, z, 0) for x in n for z in n])
        spread.append([place(y, k, z, 1) for y in n for z in n])
    return feature, copies, spread


FEATURE, COPIES, SPREAD = groups()


def shifted(value, rings, step):
    pairs = [(g[(i + step) % SIDE], g[i]) for g in rings for i in range(SIDE)]
    return lax.ppermute(value, AXES, pairs)


def grouped(value, rings):
    return lax.all_to_all(value, AXES, 0, 0, axis_index_groups=rings, tiled=True)


def other_core(value):
    return lax.ppermute(value, "c", [(0, 1), (1, 0)])


def iota(shape, dim):
    return lax.broadcasted_iota(jnp.int32, shape, dim)


def dot(a, b):
    return jnp.dot(a, b, preferred_element_type=F32)


def dot_nt(a, b):
    return lax.dot_general(a, b, (((1,), (1,)), ((), ())), preferred_element_type=F32)


def call(body, outs, args, scratch=(), smem=1, limit=16, hbm=False):
    near = pl.BlockSpec(memory_space=pltpu.VMEM)
    small, large = args[:smem], args[smem:]
    large = [pltpu.with_memory_space_constraint(a, pltpu.VMEM) for a in large]
    place_out = jax.ShapeDtypeStruct if hbm else pltpu.VMEM
    return pl.pallas_call(
        body,
        out_shape=[place_out(dims, BF) for dims in outs],
        in_specs=[pl.BlockSpec(memory_space=pltpu.SMEM)] * smem + [near] * len(large),
        out_specs=[near] * len(outs),
        scratch_shapes=[pltpu.VMEM(dims, BF) for dims in scratch],
        compiler_params=pltpu.CompilerParams(vmem_limit_bytes=limit * 2**20),
    )(*small, *large)


def column(kind, near, group, k):
    turned = (near + k) % SIDE
    return jnp.where(kind == 0, turned * SIDE + group, group * SIDE + turned)


def row_targets(route, kind):
    count = route.shape[0]
    hits = (iota((count, 8), 1) == route).astype(F32)
    earlier = (iota((count, count), 1) < iota((count, count), 0)).astype(BF)
    slot = jnp.sum(dot(earlier, hits.astype(BF)) * hits, axis=1, keepdims=True).astype(jnp.int32)
    return jnp.where(route % 2 == kind, (route // 2) * PAIR + slot, -PAIR)


def routes_of(*metas):
    return jnp.concatenate([m[:, 0:1] for m in metas], axis=0).astype(F32).astype(jnp.int32)


def pack_body(pos, meta_a, meta_b, tok_a, tok_b, cot_a, cot_b, out):
    kind, near = pos[0], pos[1]
    target = row_targets(routes_of(meta_a, meta_b), kind)
    rows = iota((2 * TOK, SENT), 1)
    pick_x = jnp.transpose((rows == target).astype(F32)).astype(BF)
    pick_y = jnp.transpose((rows == target + SLOT).astype(F32)).astype(BF)
    weight = jnp.concatenate([meta_a[:, 1:2], meta_b[:, 1:2]], axis=0).astype(F32)
    for d in range(SIDE):
        for k in range(SIDE):
            at = pl.ds(pl.multiple_of(column(kind, near, d, k) * BLK, BLK), BLK)
            x = jnp.concatenate([tok_a[:, at], tok_b[:, at]], axis=0)
            y = jnp.concatenate([cot_a[:, at], cot_b[:, at]], axis=0).astype(F32)
            y = (y * weight).astype(BF)
            out[d, :, k * BLK : (k + 1) * BLK] = (dot(pick_x, x) + dot(pick_y, y)).astype(BF)


def project_body(pos, got, w0, w1, w2a, w2b, w3, part, x_out, y_out, w2):
    at = pos[2]
    half = w2a.shape[0]
    w2[0:half, :] = w2a[...]
    w2[half:, :] = w2b[...]
    q, r = iota((SHARE, SENT), 0), iota((SHARE, SENT), 1)
    home = q + (q // SLOT) * SLOT
    take_x = (r == home).astype(BF)
    take_y = (r == home + SLOT).astype(BF)
    for k in range(SIDE):
        rows = got[(at + k) % SIDE]
        x_out[k * SHARE : (k + 1) * SHARE, :] = dot(take_x, rows).astype(BF)
        y_out[k * SHARE : (k + 1) * SHARE, :] = dot(take_y, rows).astype(BF)
    for t, left in enumerate((x_out, x_out, y_out)):
        for n in range(FF // BLK):
            cols = slice(n * BLK, (n + 1) * BLK)
            total = sum(
                dot(left[:, k * BLK : (k + 1) * BLK], w[t * BLK : (t + 1) * BLK, cols])
                for k, w in enumerate((w0, w1, w2, w3))
            ).astype(BF)
            for k in range(SIDE):
                part[(at + k) % SIDE, :, t * FF + n * BLK : t * FF + (n + 1) * BLK] = total[
                    k * SHARE : (k + 1) * SHARE
                ]


def activate_body(terms, out):
    for n in range(FF // BLK):
        def summed(t):
            cols = slice(t * FF + n * BLK, t * FF + (n + 1) * BLK)
            return sum(terms[s, :, cols].astype(F32) for s in range(SIDE))

        gate, upper, dact = summed(0), summed(1), summed(2)
        sig = jax.nn.sigmoid(gate)
        act = gate * sig * upper
        dgate = dact * upper * sig * (1.0 + gate * (1.0 - sig))
        dup = dact * gate * sig
        for t, v in enumerate((act, dgate, dup)):
            out[:, t * FF + n * BLK : t * FF + (n + 1) * BLK] = v.astype(BF)


def turn_body(x, y, xt, yt):
    for src, dst in ((x, xt), (y, yt)):
        for k in range(SIDE):
            cols = slice(k * BLK, (k + 1) * BLK)
            dst[cols, :] = jnp.transpose(src[:, cols].astype(F32)).astype(BF)


def block_grads(k, xt, yt, acts):
    cols = slice(k * BLK, (k + 1) * BLK)
    return (
        dot(xt[cols, :], acts[:, FF : 2 * FF]),
        dot(xt[cols, :], acts[:, 2 * FF : 3 * FF]),
        dot(yt[cols, :], acts[:, 0:FF]),
    )


def far_grads_body(xt, yt, a0, a1, a2, a3, acts, top, low):
    for k, a in enumerate((a0, a1, a2, a3)):
        acts[k * SHARE : (k + 1) * SHARE, :] = a[...]
    gate, upper, down = block_grads(2, xt, yt, acts)
    half = BLK // 2
    top[0:BLK, :] = gate.astype(BF)
    top[BLK : BLK + half, :] = upper[0:half].astype(BF)
    low[0:half, :] = upper[half:].astype(BF)
    low[half:, :] = down.astype(BF)


def near_grads_body(xt, yt, acts, top, low, g0, g1, g3):
    half = BLK // 2
    for t, v in enumerate(block_grads(0, xt, yt, acts)):
        g0[t * BLK : (t + 1) * BLK, :] = v.astype(BF)
    gate, upper, down = block_grads(1, xt, yt, acts)
    g1[0:BLK, :] = (gate + top[0:BLK, :].astype(F32)).astype(BF)
    g1[BLK : BLK + half, :] = (upper[0:half] + top[BLK:, :].astype(F32)).astype(BF)
    g1[BLK + half : 2 * BLK, :] = upper[half:].astype(BF)
    g1[2 * BLK :, :] = down.astype(BF)
    gate, upper, down = block_grads(3, xt, yt, acts)
    g3[0:BLK, :] = gate.astype(BF)
    g3[BLK : BLK + half, :] = upper[0:half].astype(BF)
    g3[BLK + half : 2 * BLK, :] = (upper[half:] + low[0:half, :].astype(F32)).astype(BF)
    g3[2 * BLK :, :] = (down + low[half:, :].astype(F32)).astype(BF)


def return_body(pos, acts, w0, w1, w2, w3, back, res, slot):
    at = pos[2]
    for k, w in enumerate((w0, w1, w2, w3)):
        cols = slice(k * BLK, (k + 1) * BLK)
        res[:, cols] = dot_nt(acts[:, 0:FF], w[2 * BLK : 3 * BLK, :]).astype(BF)
        grad = dot_nt(acts[:, FF : 2 * FF], w[0:BLK, :]) + dot_nt(acts[:, 2 * FF : 3 * FF], w[BLK : 2 * BLK, :])
        slot[:, cols] = grad.astype(BF)
    r, q = iota((SENT, SHARE), 0), iota((SENT, SHARE), 1)
    home = q + (q // SLOT) * SLOT
    give_m = (r == home).astype(BF)
    give_s = (r == home + SLOT).astype(BF)
    for k in range(SIDE):
        rows = slice(k * SHARE, (k + 1) * SHARE)
        back[(at + k) % SIDE] = (dot(give_m, res[rows, :]) + dot(give_s, slot[rows, :])).astype(BF)


def unpack_body(pos, meta_a, meta_b, own, oth, mixed, grad):
    kind, near, across = pos[0], pos[1], pos[2]
    mine = row_targets(routes_of(meta_a, meta_b), kind)[0:TOK]
    theirs = row_targets(routes_of(meta_b, meta_a), 1 - kind)[TOK:]
    rows = iota((TOK, SENT), 1)
    own_m, own_s = (rows == mine).astype(BF), (rows == mine + SLOT).astype(BF)
    oth_m, oth_s = (rows == theirs).astype(BF), (rows == theirs + SLOT).astype(BF)
    weight = meta_a[:, 1:2].astype(F32)
    for b in range(SIDE * SIDE):
        major, minor = b // SIDE, b % SIDE
        own_d = jnp.where(kind == 0, minor, major)
        own_k = (jnp.where(kind == 0, major, minor) - near + SIDE) % SIDE
        oth_d = jnp.where(kind == 0, major, minor)
        oth_k = (jnp.where(kind == 0, minor, major) - across + SIDE) % SIDE
        o = own[own_d, :, pl.ds(pl.multiple_of(own_k * BLK, BLK), BLK)]
        t = oth[oth_d, :, pl.ds(pl.multiple_of(oth_k * BLK, BLK), BLK)]
        cols = slice(b * BLK, (b + 1) * BLK)
        mixed[:, cols] = ((dot(own_m, o) + dot(oth_m, t)) * weight).astype(BF)
        grad[:, cols] = (dot(own_s, o) + dot(oth_s, t)).astype(BF)


def total_body(g0, g1, g3, gate, upper, down):
    def total(t):
        rows = slice(t * BLK, (t + 1) * BLK)
        return sum(g[rows, :].astype(F32) for g in (g0, g1, g3))

    gate[...] = total(0).astype(BF)
    upper[...] = total(1).astype(BF)
    down[...] = jnp.transpose(total(2)).astype(BF)


def layer(tokens, probs, routes, w_gate, w_up, w_down, cotangent):
    y, x, c = lax.axis_index("y"), lax.axis_index("x"), lax.axis_index("c")
    pos = jnp.stack([c, jnp.where(c == 0, y, x), jnp.where(c == 0, x, y)]).astype(jnp.int32)
    meta = jnp.concatenate([routes.astype(BF), probs], axis=1)
    meta_b, tok_b, cot_b = other_core(meta), other_core(tokens), other_core(cotangent)
    w0 = jnp.concatenate([w_gate[0], w_up[0], w_down[0].T], axis=0)
    half = w0.shape[0] // 2
    w1, w3 = shifted(w0, COPIES, 1), shifted(w0, COPIES, -1)
    (sent,) = call(pack_body, [(SIDE, SENT, WIDE)], [pos, meta, meta_b, tokens, tok_b, cotangent, cot_b])
    w2a, w2b = shifted(w1[:half], COPIES, 1), shifted(w3[half:], COPIES, -1)
    got = grouped(sent.reshape(SIDE * SIDE, PAIR, WIDE), SPREAD).reshape(SIDE, SENT, WIDE)
    part, rows_x, rows_y, w2 = call(
        project_body,
        [(SIDE, SHARE, 3 * FF), (ROWS, WIDE), (ROWS, WIDE), (3 * BLK, FF)],
        [pos, got, w0, w1, w2a, w2b, w3],
    )
    terms = grouped(part, FEATURE)
    (a0,) = call(activate_body, [(SHARE, 3 * FF)], [terms], smem=0)
    a1, a2, a3 = [shifted(a0, FEATURE, k) for k in (1, 2, -1)]
    xt, yt = call(turn_body, [(WIDE, ROWS), (WIDE, ROWS)], [rows_x, rows_y], smem=0)
    acts, top, low = call(
        far_grads_body,
        [(ROWS, 3 * FF), (half, FF), (half, FF)],
        [xt, yt, a0, a1, a2, a3],
        smem=0,
    )
    top, low = shifted(top, COPIES, -1), shifted(low, COPIES, 1)
    (back,) = call(
        return_body,
        [(SIDE, SENT, WIDE)],
        [pos, acts, w0, w1, w2, w3],
        scratch=[(ROWS, WIDE), (ROWS, WIDE)],
    )
    own = grouped(back.reshape(SIDE * SIDE, PAIR, WIDE), SPREAD).reshape(SIDE, SENT, WIDE)
    g0, g1, g3 = call(near_grads_body, [(3 * BLK, FF)] * 3, [xt, yt, acts, top, low], smem=0)
    g1, g3 = shifted(g1, COPIES, -1), shifted(g3, COPIES, 1)
    oth = other_core(own)
    mixed, grad = call(
        unpack_body, [(TOK, SIDE * WIDE)] * 2, [pos, meta, meta_b, own, oth], hbm=True
    )
    gate, upper, down = call(
        total_body, [(BLK, FF), (BLK, FF), (FF, BLK)], [g0, g1, g3], smem=0, hbm=True
    )
    return mixed, grad, gate[None], upper[None], down[None]


def solution(mesh):
    finer = Mesh(mesh.devices.reshape(SIDE, SIDE, SIDE, 2), AXES)
    rows = P(AXES, None)
    wide = P(("z", "c"), ("y", "x"), None)
    tall = P(("z", "c"), None, ("y", "x"))
    return jax.shard_map(
        layer,
        mesh=finer,
        in_specs=(rows, rows, rows, wide, wide, tall, rows),
        out_specs=(rows, rows, wide, wide, tall),
        check_vma=False,
    )
```

```python
import jax
import jax.numpy as jnp
from jax import lax
from jax.experimental import pallas as pl
from jax.experimental.pallas import tpu as pltpu
from jax.sharding import Mesh
from jax.sharding import PartitionSpec as P


AXES = ("y", "x", "z", "c")
BF = jnp.bfloat16
F32 = jnp.float32
SIDE = 4
TOK = 128
BLK = 256
FF = 1024
SLOT = 36
PAIR = 2 * SLOT
PAD = 40
SHARE = SIDE * SLOT
SENT = SIDE * PAIR
BACK = SIDE * PAD
ROWS = SIDE * SHARE
WIDE = SIDE * BLK


def place(y, x, z, c):
    return ((y * SIDE + x) * SIDE + z) * 2 + c


def groups():
    n = range(SIDE)
    feature, copies, spread = [], [], []
    for k in n:
        for z in n:
            feature.append([place(k, x, z, 0) for x in n])
            feature.append([place(y, k, z, 1) for y in n])
            copies.append([place(y, k, z, 0) for y in n])
            copies.append([place(k, x, z, 1) for x in n])
        spread.append([place(k, x, z, 0) for x in n for z in n])
        spread.append([place(y, k, z, 1) for y in n for z in n])
    return feature, copies, spread


FEATURE, COPIES, SPREAD = groups()


def shifted(value, rings, step):
    pairs = [(g[(i + step) % SIDE], g[i]) for g in rings for i in range(SIDE)]
    return lax.ppermute(value, AXES, pairs)


def grouped(value, rings):
    return lax.all_to_all(value, AXES, 0, 0, axis_index_groups=rings, tiled=True)


def other_core(value):
    return lax.ppermute(value, "c", [(0, 1), (1, 0)])


def iota(shape, dim):
    return lax.broadcasted_iota(jnp.int32, shape, dim)


def dot(a, b):
    return jnp.dot(a, b, preferred_element_type=F32)


def dot_nt(a, b):
    return lax.dot_general(a, b, (((1,), (1,)), ((), ())), preferred_element_type=F32)


def near(value):
    return pltpu.with_memory_space_constraint(value, pltpu.VMEM)


def far(value):
    return pltpu.with_memory_space_constraint(value, pltpu.HBM)


def call(body, outs, args, hbm=(), scratch=(), smem=1, limit=16):
    vmem = pl.BlockSpec(memory_space=pltpu.VMEM)
    shapes = [(pltpu.HBM if n in hbm else pltpu.VMEM)(dims, BF) for n, dims in enumerate(outs)]
    return pl.pallas_call(
        body,
        out_shape=shapes,
        in_specs=[pl.BlockSpec(memory_space=pltpu.SMEM)] * smem + [vmem] * (len(args) - smem),
        out_specs=[vmem] * len(outs),
        scratch_shapes=[pltpu.VMEM(dims, BF) for dims in scratch],
        compiler_params=pltpu.CompilerParams(vmem_limit_bytes=limit * 2**20),
    )(*args)


def column(kind, near, group, k):
    turned = (near + k) % SIDE
    return jnp.where(kind == 0, turned * SIDE + group, group * SIDE + turned)


def row_targets(route, kind, block):
    count = route.shape[0]
    hits = (iota((count, 8), 1) == route).astype(F32)
    earlier = (iota((count, count), 1) < iota((count, count), 0)).astype(BF)
    slot = jnp.sum(dot(earlier, hits.astype(BF)) * hits, axis=1, keepdims=True).astype(jnp.int32)
    return jnp.where(route % 2 == kind, (route // 2) * block + slot, -2 * block)


def routes_of(*metas):
    return jnp.concatenate([m[:, 0:1] for m in metas], axis=0).astype(F32).astype(jnp.int32)


def pack_body(pos, meta_a, meta_b, tok_a, tok_b, cot_a, cot_b, out):
    kind, at = pos[0], pos[1]
    target = row_targets(routes_of(meta_a, meta_b), kind, PAIR)
    rows = iota((2 * TOK, SENT), 1)
    pick_x = jnp.transpose((rows == target).astype(F32)).astype(BF)
    pick_y = jnp.transpose((rows == target + SLOT).astype(F32)).astype(BF)
    weight = jnp.concatenate([meta_a[:, 1:2], meta_b[:, 1:2]], axis=0).astype(F32)
    for d in range(SIDE):
        for k in range(SIDE):
            src = pl.ds(pl.multiple_of(column(kind, at, d, k) * BLK, BLK), BLK)
            x = jnp.concatenate([tok_a[:, src], tok_b[:, src]], axis=0)
            y = jnp.concatenate([cot_a[:, src], cot_b[:, src]], axis=0).astype(F32)
            both = dot(pick_x, x) + dot(pick_y, (y * weight).astype(BF))
            out[d, :, k * BLK : (k + 1) * BLK] = both.astype(BF)


def compact(pos, got, first, rows_out):
    q, r = iota((SHARE, SENT), 0), iota((SHARE, SENT), 1)
    take = (r == q + (q // SLOT) * (PAIR - SLOT) + first).astype(BF)
    for k in range(SIDE):
        rows_out[k * SHARE : (k + 1) * SHARE, :] = dot(take, got[(pos[2] + k) % SIDE]).astype(BF)


def expand(pos, rows, back):
    r, q = iota((BACK, SHARE), 0), iota((BACK, SHARE), 1)
    give = (r == q + (q // SLOT) * (PAD - SLOT)).astype(BF)
    for k in range(SIDE):
        back[(pos[2] + k) % SIDE] = dot(give, rows[k * SHARE : (k + 1) * SHARE, :]).astype(BF)


def share_out(total, parts, cols):
    total = total.astype(BF)
    for k, part in enumerate(parts):
        part[:, cols] = total[k * SHARE : (k + 1) * SHARE]


def project_y_body(pos, got, d0, d1, d2, d3, rows, p0, p1, p2, p3):
    compact(pos, got, SLOT, rows)
    for n in range(FF // BLK):
        cols = slice(n * BLK, (n + 1) * BLK)
        total = sum(dot_nt(rows[:, k * BLK : (k + 1) * BLK], w[cols, :]) for k, w in enumerate((d0, d1, d2, d3)))
        share_out(total, (p0, p1, p2, p3), cols)


def project_x_body(pos, got, w0, w1, w2, w3, rows, p0, p1, p2, p3):
    compact(pos, got, 0, rows)
    for n in range(2 * FF // BLK):
        t, cols = divmod(n * BLK, FF)
        total = sum(
            dot(rows[:, k * BLK : (k + 1) * BLK], w[t * BLK : (t + 1) * BLK, cols : cols + BLK])
            for k, w in enumerate((w0, w1, w2, w3))
        )
        share_out(total, (p0, p1, p2, p3), slice(n * BLK, (n + 1) * BLK))


def activate_body(y0, y1, y2, y3, x0, x1, x2, x3, act, grads):
    for n in range(FF // BLK):
        cols = slice(n * BLK, (n + 1) * BLK)
        ups = slice(FF + n * BLK, FF + (n + 1) * BLK)
        gate = sum(p[:, cols].astype(F32) for p in (x0, x1, x2, x3))
        upper = sum(p[:, ups].astype(F32) for p in (x0, x1, x2, x3))
        dact = sum(p[:, cols].astype(F32) for p in (y0, y1, y2, y3))
        sig = jax.nn.sigmoid(gate)
        act[:, cols] = (gate * sig * upper).astype(BF)
        grads[:, cols] = (dact * upper * sig * (1.0 + gate * (1.0 - sig))).astype(BF)
        grads[:, ups] = (dact * gate * sig).astype(BF)


def turn_body(x, y, xt, yt):
    for src, dst in ((x, xt), (y, yt)):
        for k in range(SIDE):
            cols = slice(k * BLK, (k + 1) * BLK)
            dst[cols, :] = jnp.transpose(src[:, cols].astype(F32)).astype(BF)


def result_body(pos, a0, a1, a2, a3, d0, d1, d2, d3, back, acts, res):
    for k, a in enumerate((a0, a1, a2, a3)):
        acts[k * SHARE : (k + 1) * SHARE, :] = a[...]
    for k, w in enumerate((d0, d1, d2, d3)):
        res[:, k * BLK : (k + 1) * BLK] = dot(acts[...], w[...]).astype(BF)
    expand(pos, res, back)


def grads_body(xt, yt, acts, a0, a1, a2, a3, grads, n0, n1, n2, n3):
    for k, a in enumerate((a0, a1, a2, a3)):
        grads[k * SHARE : (k + 1) * SHARE, :] = a[...]
    for k, out in ((2, n2), (1, n1), (3, n3), (0, n0)):
        rows = slice(k * BLK, (k + 1) * BLK)
        out[0:BLK, :] = dot(xt[rows, :], grads[:, 0:FF]).astype(BF)
        out[BLK : 2 * BLK, :] = dot(xt[rows, :], grads[:, FF:]).astype(BF)
        out[2 * BLK :, :] = dot(yt[rows, :], acts[...]).astype(BF)


def slot_body(pos, grads, w0, w1, w2, w3, back, slot):
    for k, w in enumerate((w0, w1, w2, w3)):
        total = dot_nt(grads[:, 0:FF], w[0:BLK, :]) + dot_nt(grads[:, FF:], w[BLK:, :])
        slot[:, k * BLK : (k + 1) * BLK] = total.astype(BF)
    expand(pos, slot, back)


def unpack_body(pos, meta_a, meta_b, own_m, own_s, oth_m, oth_s, mixed, grad):
    kind, at, across = pos[0], pos[1], pos[2]
    mine = row_targets(routes_of(meta_a, meta_b), kind, PAD)[0:TOK]
    theirs = row_targets(routes_of(meta_b, meta_a), 1 - kind, PAD)[TOK:]
    rows = iota((TOK, BACK), 1)
    mine, theirs = (rows == mine).astype(BF), (rows == theirs).astype(BF)
    weight = meta_a[:, 1:2].astype(F32)
    for b in range(SIDE * SIDE):
        major, minor = b // SIDE, b % SIDE
        own_d = jnp.where(kind == 0, minor, major)
        own_k = (jnp.where(kind == 0, major, minor) - at + SIDE) % SIDE
        oth_d = jnp.where(kind == 0, major, minor)
        oth_k = (jnp.where(kind == 0, minor, major) - across + SIDE) % SIDE
        own_c = pl.ds(pl.multiple_of(own_k * BLK, BLK), BLK)
        oth_c = pl.ds(pl.multiple_of(oth_k * BLK, BLK), BLK)
        cols = slice(b * BLK, (b + 1) * BLK)
        total = dot(mine, own_m[own_d, :, own_c]) + dot(theirs, oth_m[oth_d, :, oth_c])
        mixed[:, cols] = (total * weight).astype(BF)
        total = dot(mine, own_s[own_d, :, own_c]) + dot(theirs, oth_s[oth_d, :, oth_c])
        grad[:, cols] = total.astype(BF)


def total_body(n0, n1, n2, n3, gate, upper, down):
    def total(t):
        rows = slice(t * BLK, (t + 1) * BLK)
        return sum(n[rows, :].astype(F32) for n in (n0, n1, n2, n3))

    gate[...] = total(0).astype(BF)
    upper[...] = total(1).astype(BF)
    down[...] = jnp.transpose(total(2)).astype(BF)


def exchanged(value, block):
    rows = value.reshape(SIDE * SIDE, block, WIDE)
    return grouped(rows, SPREAD).reshape(SIDE, SIDE * block, WIDE)


def layer(tokens, probs, routes, w_gate, w_up, w_down, cotangent):
    y, x, c = lax.axis_index("y"), lax.axis_index("x"), lax.axis_index("c")
    pos = jnp.stack([c, jnp.where(c == 0, y, x), jnp.where(c == 0, x, y)]).astype(jnp.int32)
    meta = jnp.concatenate([routes.astype(BF), probs], axis=1)
    meta_b, tok_b, cot_b = other_core(meta), other_core(tokens), other_core(cotangent)
    d0, w0 = w_down[0], jnp.concatenate([w_gate[0], w_up[0]], axis=0)
    d1, d3 = far(shifted(d0, COPIES, 1)), far(shifted(d0, COPIES, -1))
    w1, w3 = far(shifted(w0, COPIES, 1)), far(shifted(w0, COPIES, -1))
    d2, w2 = far(shifted(d1, COPIES, 1)), far(shifted(w3, COPIES, -1))
    ds, ws = [far(d0), d1, d2, d3], [far(w0), w1, w2, w3]
    (sent,) = call(
        pack_body,
        [(SIDE, SENT, WIDE)],
        [pos, meta, meta_b, far(tokens), near(tok_b), far(cotangent), near(cot_b)],
        hbm=(0,),
    )
    got = near(exchanged(sent, PAIR))
    rows_x, *px = call(project_x_body, [(ROWS, WIDE)] + [(SHARE, 2 * FF)] * 4, [pos, got, *ws])
    px = [px[0]] + [near(shifted(px[k], FEATURE, -k)) for k in (1, 2, 3)]
    rows_y, *py = call(project_y_body, [(ROWS, WIDE)] + [(SHARE, FF)] * 4, [pos, got, *ds])
    py = [py[0]] + [near(shifted(py[k], FEATURE, -k)) for k in (1, 2, 3)]
    act, grad = call(activate_body, [(SHARE, FF), (SHARE, 2 * FF)], [*py, *px], smem=0)
    act = [act] + [near(shifted(act, FEATURE, k)) for k in (1, 2, -1)]
    grad = [far(grad)] + [far(shifted(grad, FEATURE, k)) for k in (1, 2, -1)]
    xt, yt = call(turn_body, [(WIDE, ROWS)] * 2, [rows_x, rows_y], smem=0, hbm=(0, 1))
    back_m, acts = call(
        result_body, [(SIDE, BACK, WIDE), (ROWS, FF)], [pos, *act, *ds], hbm=(0, 1), scratch=[(ROWS, WIDE)]
    )
    own_m = exchanged(back_m, PAD)
    grads, *ns = call(
        grads_body,
        [(ROWS, 2 * FF)] + [(3 * BLK, FF)] * 4,
        [far(xt), far(yt), far(acts), *grad],
        smem=0,
        hbm=(1, 2, 3, 4),
        limit=24,
    )
    ns = [far(ns[0])] + [near(shifted(ns[k], COPIES, -k)) for k in (1, 2, 3)]
    (back_s,) = call(slot_body, [(SIDE, BACK, WIDE)], [pos, near(grads), *ws], hbm=(0,), scratch=[(ROWS, WIDE)])
    own_s = exchanged(back_s, PAD)
    oth_m = near(other_core(own_m))
    oth_s = near(other_core(own_s))
    mixed, into = call(
        unpack_body,
        [(TOK, SIDE * WIDE)] * 2,
        [pos, meta, meta_b, far(own_m), far(own_s), oth_m, oth_s],
        hbm=(0, 1),
    )
    gate, upper, down = call(total_body, [(BLK, FF), (BLK, FF), (FF, BLK)], ns, smem=0, hbm=(0, 1, 2))
    return mixed, into, gate[None], upper[None], down[None]


def solution(mesh):
    finer = Mesh(mesh.devices.reshape(SIDE, SIDE, SIDE, 2), AXES)
    rows = P(AXES, None)
    wide = P(("z", "c"), ("y", "x"), None)
    tall = P(("z", "c"), None, ("y", "x"))
    return jax.shard_map(
        layer,
        mesh=finer,
        in_specs=(rows, rows, rows, wide, wide, tall, rows),
        out_specs=(rows, rows, wide, wide, tall),
        check_vma=False,
    )
```

```python
import functools

import jax
import jax.numpy as jnp
from jax import lax
from jax.experimental import pallas as pl
from jax.experimental.pallas import tpu as pltpu
from jax.sharding import Mesh
from jax.sharding import PartitionSpec as P


AXES = ("y", "x", "z", "c")
BF = jnp.bfloat16
F32 = jnp.float32
SIDE = 4
TOK = 128
BLK = 256
FF = 1024
SLOT = 36
PAIR = 2 * SLOT
PART = SLOT // 2
SHARE = SIDE * PART
SENT = SIDE * PAIR
ROWS = SIDE * SHARE
WIDE = SIDE * BLK


def place(y, x, z, c):
    return ((y * SIDE + x) * SIDE + z) * 2 + c


def groups():
    n = range(SIDE)
    feature, copies, spread = [], [], []
    for k in n:
        for z in n:
            feature.append([place(k, x, z, 0) for x in n])
            feature.append([place(y, k, z, 1) for y in n])
            copies.append([place(y, k, z, 0) for y in n])
            copies.append([place(k, x, z, 1) for x in n])
        spread.append([place(k, x, z, 0) for x in n for z in n])
        spread.append([place(y, k, z, 1) for y in n for z in n])
    return feature, copies, spread


FEATURE, COPIES, SPREAD = groups()


def shifted(value, rings, step):
    pairs = [(g[(i + step) % SIDE], g[i]) for g in rings for i in range(SIDE)]
    return lax.ppermute(value, AXES, pairs)


def grouped(value, rings):
    return lax.all_to_all(value, AXES, 0, 0, axis_index_groups=rings, tiled=True)


def other_core(value):
    return lax.ppermute(value, "c", [(0, 1), (1, 0)])


def iota(shape, dim):
    return lax.broadcasted_iota(jnp.int32, shape, dim)


def dot(a, b):
    return jnp.dot(a, b, preferred_element_type=F32)


def dot_nt(a, b):
    return lax.dot_general(a, b, (((1,), (1,)), ((), ())), preferred_element_type=F32)


def near(value):
    return pltpu.with_memory_space_constraint(value, pltpu.VMEM)


def far(value):
    return pltpu.with_memory_space_constraint(value, pltpu.HBM)


def call(body, outs, args, hbm=(), scratch=(), copies=0, smem=1, limit=20):
    vmem, raw = pl.BlockSpec(memory_space=pltpu.VMEM), pl.BlockSpec(memory_space=pl.ANY)
    specs = [pl.BlockSpec(memory_space=pltpu.SMEM)] * smem
    specs += [raw if isinstance(a, tuple) else vmem for a in args[smem:]]
    held = [pltpu.VMEM(dims, BF) for dims in scratch]
    return pl.pallas_call(
        body,
        out_shape=[(pltpu.HBM if n in hbm else pltpu.VMEM)(dims, BF) for n, dims in enumerate(outs)],
        in_specs=specs,
        out_specs=[raw if n in hbm else vmem for n in range(len(outs))],
        scratch_shapes=held + ([pltpu.SemaphoreType.DMA((copies,))] if copies else []),
        compiler_params=pltpu.CompilerParams(vmem_limit_bytes=limit * 2**20),
    )(*[far(a[0]) if isinstance(a, tuple) else a for a in args])


class Copies:
    def __init__(self, sems):
        self.sems, self.count, self.going = sems, 0, []

    def start(self, src, dst):
        copy = pltpu.make_async_copy(src, dst, self.sems.at[self.count])
        copy.start()
        self.count += 1
        return copy

    def send(self, src, dst):
        self.going.append(self.start(src, dst))

    def drain(self):
        for copy in self.going:
            copy.wait()


def column(kind, near, group, k):
    turned = (near + k) % SIDE
    return jnp.where(kind == 0, turned * SIDE + group, group * SIDE + turned)


def slots(route):
    count = route.shape[0]
    hits = (iota((count, 8), 1) == route).astype(F32)
    earlier = (iota((count, count), 1) < iota((count, count), 0)).astype(BF)
    return jnp.sum(dot(earlier, hits.astype(BF)) * hits, axis=1, keepdims=True).astype(jnp.int32)


def routes_of(*metas):
    return jnp.concatenate([m[:, 0:1] for m in metas], axis=0).astype(F32).astype(jnp.int32)


def pack_body(pos, meta_a, meta_b, tok_b, cot_b, tok_far, cot_far, out_far, tok_a, cot_a, out, sems):
    kind, at = pos[0], pos[1]
    copies = Copies(sems)
    loads = [copies.start(tok_far, tok_a), copies.start(cot_far, cot_a)]
    route = routes_of(meta_a, meta_b)
    target = jnp.where(route % 2 == kind, (route // 2) * PAIR + slots(route), -PAIR)
    rows = iota((2 * TOK, SENT), 1)
    pick_x = jnp.transpose((rows == target).astype(F32)).astype(BF)
    pick_y = jnp.transpose((rows == target + SLOT).astype(F32)).astype(BF)
    weight = jnp.concatenate([meta_a[:, 1:2], meta_b[:, 1:2]], axis=0).astype(F32)
    for load in loads:
        load.wait()
    for d in range(SIDE):
        for k in range(SIDE):
            src = pl.ds(pl.multiple_of(column(kind, at, d, k) * BLK, BLK), BLK)
            x = jnp.concatenate([tok_a[:, src], tok_b[:, src]], axis=0)
            y = jnp.concatenate([cot_a[:, src], cot_b[:, src]], axis=0).astype(F32)
            both = dot(pick_x, x) + dot(pick_y, (y * weight).astype(BF))
            out[d, :, k * BLK : (k + 1) * BLK] = both.astype(BF)
        copies.send(out.at[d], out_far.at[d])
    copies.drain()


def project_body(first, loads, pos, got, *refs):
    if loads:
        given, x, y, parts, kept, sems = refs[:13], refs[13], refs[14], refs[15:19], refs[19:27], refs[27]
        copies = Copies(sems)
        d0, d1, low, high, d3 = given[:5]
        halves = (slice(0, FF // 2), slice(FF // 2, FF))
        going = [copies.start(a, kept[k]) for k, a in ((0, d0), (1, d1), (3, d3))]
        going += [copies.start(a, kept[2].at[rows, :]) for a, rows in zip((low, high), halves)]
        first_up = len(going)
        for t in range(2):
            for k in range(SIDE):
                rows = slice(t * BLK, (t + 1) * BLK)
                going.append(copies.start(given[5 + t * SIDE + k], kept[SIDE + k].at[rows, :]))
    else:
        kept, x, y, parts = refs[:8], refs[8], refs[9], refs[10:14]
    ds, ws = kept[:SIDE], kept[SIDE:]
    q, r = iota((SHARE, SENT), 0), iota((SHARE, SENT), 1)
    home = q + (q // PART) * (PAIR - PART) + first
    for rows, take in ((x, (r == home).astype(BF)), (y, (r == home + SLOT).astype(BF))):
        for k in range(SIDE):
            rows[k * SHARE : (k + 1) * SHARE, :] = dot(take, got[(pos[2] + k) % SIDE]).astype(BF)
    for t in (2, 0, 1):
        if loads and t != 1:
            for copy in going[:first_up] if t == 2 else going[first_up:]:
                copy.wait()
        for n in range(FF // BLK):
            cols = slice(n * BLK, (n + 1) * BLK)
            total = 0.0
            for k in range(SIDE):
                block = slice(k * BLK, (k + 1) * BLK)
                if t == 2:
                    total = total + dot_nt(y[:, block], ds[k][cols, :])
                else:
                    total = total + dot(x[:, block], ws[k][t * BLK : (t + 1) * BLK, cols])
            total = total.astype(BF)
            for k, p in enumerate(parts):
                p[:, t * FF + n * BLK : t * FF + (n + 1) * BLK] = total[k * SHARE : (k + 1) * SHARE]


def activate_body(p0, p1, p2, p3, out):
    for n in range(FF // BLK):
        cols = [slice(t * FF + n * BLK, t * FF + (n + 1) * BLK) for t in range(3)]
        gate, upper, dact = [sum(p[:, c].astype(F32) for p in (p0, p1, p2, p3)) for c in cols]
        sig = jax.nn.sigmoid(gate)
        out[:, cols[0]] = (gate * sig * upper).astype(BF)
        out[:, cols[1]] = (dact * upper * sig * (1.0 + gate * (1.0 - sig))).astype(BF)
        out[:, cols[2]] = (dact * gate * sig).astype(BF)


def turn_body(x_a, x_b, y_a, y_b, xt, yt, own_far, sems):
    copies = Copies(sems)
    for n, (a, b, out) in enumerate(((x_a, x_b, xt), (y_a, y_b, yt))):
        for k in range(SIDE):
            cols = slice(k * BLK, (k + 1) * BLK)
            both = [v[m * SHARE : (m + 1) * SHARE, cols].astype(F32) for m in range(SIDE) for v in (a, b)]
            both = jnp.concatenate(both, axis=0)
            out[cols, :] = jnp.transpose(both).astype(BF)
        copies.send(out.at[0:BLK, :], own_far.at[n])
    copies.drain()


def block_grads(out, x, y, acts):
    out[0:BLK, :] = dot(x, acts[:, FF : 2 * FF]).astype(BF)
    out[BLK : 2 * BLK, :] = dot(x, acts[:, 2 * FF :]).astype(BF)
    out[2 * BLK :, :] = dot(y, acts[:, 0:FF]).astype(BF)


def first_grads_body(xt, yt, *refs):
    pieces, acts, out_far, out, sems = refs[: 2 * SIDE], *refs[2 * SIDE :]
    copies = Copies(sems)
    for n, a in enumerate(pieces):
        at = 2 * (n % SIDE) + n // SIDE
        acts[at * SHARE : (at + 1) * SHARE, :] = a[...]
    rows = slice(2 * BLK, 3 * BLK)
    block_grads(out, xt[rows, :], yt[rows, :], acts)
    copies.send(out, out_far)
    copies.drain()


def more_grads_body(xt, yt, acts, acts_far, one_far, three_far, one, three, sems):
    copies = Copies(sems)
    copies.send(acts, acts_far)
    for k, out, out_far in ((1, one, one_far), (3, three, three_far)):
        rows = slice(k * BLK, (k + 1) * BLK)
        block_grads(out, xt[rows, :], yt[rows, :], acts)
        copies.send(out, out_far)
    copies.drain()


def own_grads_body(turned_far, acts_far, out, turned, acts, sems):
    copies = Copies(sems)
    loads = [copies.start(turned_far, turned), copies.start(acts_far, acts)]
    for load in loads:
        load.wait()
    block_grads(out, turned[0], turned[1], acts)


def return_body(pos, acts, *refs):
    weights, back_far, res, slot, back, sems = refs[: 2 * SIDE], *refs[2 * SIDE :]
    copies = Copies(sems)
    for k in range(SIDE):
        d, w, cols = weights[k], weights[SIDE + k], slice(k * BLK, (k + 1) * BLK)
        res[:, cols] = dot(acts[:, 0:FF], d[...]).astype(BF)
        total = dot_nt(acts[:, FF : 2 * FF], w[0:BLK, :]) + dot_nt(acts[:, 2 * FF :], w[BLK:, :])
        slot[:, cols] = total.astype(BF)
    r, q = iota((SENT, 2 * SHARE), 0), iota((SENT, 2 * SHARE), 1)
    step, q = q // SHARE, q % SHARE
    home = q + (q // PART) * (PAIR - PART) + step * PART
    give_m, give_s = (r == home).astype(BF), (r == home + SLOT).astype(BF)
    for k in range(SIDE):
        rows = slice(2 * k * SHARE, 2 * (k + 1) * SHARE)
        back[k] = (dot(give_m, res[rows, :]) + dot(give_s, slot[rows, :])).astype(BF)
        copies.send(back.at[k], back_far.at[(pos[2] + k) % SIDE])
    copies.drain()


def unpack_body(pos, meta_a, meta_b, own, oth, mixed_far, grad_far, mixed, grad, sems):
    kind, at, across = pos[0], pos[1], pos[2]
    copies = Copies(sems)
    rows = iota((TOK, SENT), 1)

    def picks(route, core, mine):
        target = jnp.where(route % 2 == core, (route // 2) * PAIR + slots(route), -PAIR)[mine]
        return (rows == target).astype(BF), (rows == target + SLOT).astype(BF)

    own_m, own_s = picks(routes_of(meta_a, meta_b), kind, slice(0, TOK))
    oth_m, oth_s = picks(routes_of(meta_b, meta_a), 1 - kind, slice(TOK, 2 * TOK))
    weight = meta_a[:, 1:2].astype(F32)
    for b in range(SIDE * SIDE):
        major, minor = b // SIDE, b % SIDE
        own_d = jnp.where(kind == 0, minor, major)
        own_k = (jnp.where(kind == 0, major, minor) - at + SIDE) % SIDE
        oth_d = jnp.where(kind == 0, major, minor)
        oth_k = (jnp.where(kind == 0, minor, major) - across + SIDE) % SIDE
        o = own[own_d, :, pl.ds(pl.multiple_of(own_k * BLK, BLK), BLK)]
        t = oth[oth_d, :, pl.ds(pl.multiple_of(oth_k * BLK, BLK), BLK)]
        cols = slice(b * BLK, (b + 1) * BLK)
        mixed[:, cols] = ((dot(own_m, o) + dot(oth_m, t)) * weight).astype(BF)
        grad[:, cols] = (dot(own_s, o) + dot(oth_s, t)).astype(BF)
        if minor == SIDE - 1:
            done = pl.ds(major * WIDE, WIDE)
            copies.send(mixed.at[:, done], mixed_far.at[:, done])
            copies.send(grad.at[:, done], grad_far.at[:, done])
    copies.drain()


def total_body(n0, n1, n2, n3, gate_far, upper_far, down_far, gate, upper, down, sems):
    copies = Copies(sems)

    def total(t):
        rows = slice(t * BLK, (t + 1) * BLK)
        return sum(n[rows, :].astype(F32) for n in (n0, n1, n2, n3))

    down[...] = jnp.transpose(total(2)).astype(BF)
    copies.send(down, down_far)
    gate[...] = total(0).astype(BF)
    copies.send(gate, gate_far)
    upper[...] = total(1).astype(BF)
    copies.send(upper, upper_far)
    copies.drain()


def exchanged(value):
    rows = value.reshape(SIDE * SIDE, PAIR, WIDE)
    return near(grouped(rows, SPREAD).reshape(SIDE, SENT, WIDE))


def layer(tokens, probs, routes, w_gate, w_up, w_down, cotangent):
    y, x, c = lax.axis_index("y"), lax.axis_index("x"), lax.axis_index("c")
    pos = jnp.stack([c, jnp.where(c == 0, y, x), jnp.where(c == 0, x, y)]).astype(jnp.int32)
    meta = jnp.concatenate([routes.astype(BF), probs], axis=1)
    meta_b, tok_b, cot_b = other_core(meta), other_core(tokens), other_core(cotangent)
    d0, g0, u0 = w_down[0], w_gate[0], w_up[0]
    g1, g3 = shifted(g0, COPIES, 1), shifted(g0, COPIES, -1)
    u1, u3 = shifted(u0, COPIES, 1), shifted(u0, COPIES, -1)
    d1, d3 = shifted(d0, COPIES, 1), shifted(d0, COPIES, -1)
    half = FF // 2
    g2 = near(shifted(g3, COPIES, -1))
    u2 = near(shifted(u1, COPIES, 1))
    low, high = near(shifted(d1[:half], COPIES, 1)), near(shifted(d3[half:], COPIES, -1))
    weights = [(d0,), (d1,), low, high, (d3,), (g0,), (g1,), g2, (g3,), (u0,), (u1,), u2, (u3,)]
    (sent,) = call(
        pack_body,
        [(SIDE, SENT, WIDE)],
        [pos, meta, meta_b, near(tok_b), near(cot_b), (tokens,), (cotangent,)],
        hbm=(0,),
        scratch=[tokens.shape, tokens.shape, (SIDE, SENT, WIDE)],
        copies=2 + SIDE,
    )
    got = exchanged(sent)
    xs, ys, parts, pieces = [], [], [], []
    kept = weights
    for p in (0, 1):
        x, y, *part = call(
            functools.partial(project_body, p * PART, p == 0),
            [(ROWS, WIDE)] * 2 + [(SHARE, 3 * FF)] * SIDE + ([] if p else [(FF, BLK)] * SIDE + [(2 * BLK, FF)] * SIDE),
            [pos, got, *kept],
            copies=0 if p else len(weights),
        )
        if p == 0:
            part, kept = part[:SIDE], part[SIDE:]
        parts.append([part[0]] + [near(shifted(part[k], FEATURE, -k)) for k in (1, 2, 3)])
        xs.append(x)
        ys.append(y)
    for p in (0, 1):
        (act,) = call(activate_body, [(SHARE, 3 * FF)], parts[p], smem=0)
        pieces += [act] + [near(shifted(act, FEATURE, k)) for k in (1, 2, -1)]
    turned = (2, BLK, 2 * ROWS)
    block = (3 * BLK, FF)
    whole = (2 * ROWS, 3 * FF)
    xt, yt, own_t = call(turn_body, [(WIDE, 2 * ROWS)] * 2 + [turned], [*xs, *ys], smem=0, hbm=(2,), copies=2)
    acts, n2 = call(first_grads_body, [whole, block], [xt, yt, *pieces], smem=0, hbm=(1,), scratch=[block], copies=1)
    n2 = near(shifted(n2, COPIES, -2))
    acts_far, n1, n3 = call(
        more_grads_body,
        [whole, block, block],
        [xt, yt, near(acts)],
        smem=0,
        hbm=(0, 1, 2),
        scratch=[block] * 2,
        copies=3,
    )
    n1, n3 = near(shifted(n1, COPIES, -1)), near(shifted(n3, COPIES, 1))
    (back,) = call(
        return_body,
        [(SIDE, SENT, WIDE)],
        [pos, near(acts), *kept],
        hbm=(0,),
        scratch=[(2 * ROWS, WIDE)] * 2 + [(SIDE, SENT, WIDE)],
        copies=SIDE,
    )
    own = exchanged(back)
    (n0,) = call(own_grads_body, [block], [(own_t,), (acts_far,)], smem=0, scratch=[turned, whole], copies=2)
    ns = [n0, n1, n2, n3]
    oth = near(other_core(own))
    mixed, into = call(
        unpack_body,
        [tokens.shape] * 2,
        [pos, meta, meta_b, own, oth],
        hbm=(0, 1),
        scratch=[tokens.shape] * 2,
        copies=2 * SIDE,
    )
    shapes = [(BLK, FF), (BLK, FF), (FF, BLK)]
    gate, upper, down = call(total_body, shapes, ns, smem=0, hbm=(0, 1, 2), scratch=shapes, copies=3)
    return mixed, into, gate[None], upper[None], down[None]


def solution(mesh):
    finer = Mesh(mesh.devices.reshape(SIDE, SIDE, SIDE, 2), AXES)
    rows = P(AXES, None)
    wide = P(("z", "c"), ("y", "x"), None)
    tall = P(("z", "c"), None, ("y", "x"))
    return jax.shard_map(
        layer,
        mesh=finer,
        in_specs=(rows, rows, rows, wide, wide, tall, rows),
        out_specs=(rows, rows, wide, wide, tall),
        check_vma=False,
    )
```

```python
import functools

import jax
import jax.numpy as jnp
from jax import lax
from jax.experimental import pallas as pl
from jax.experimental.pallas import tpu as pltpu
from jax.sharding import Mesh
from jax.sharding import PartitionSpec as P


AXES = ("y", "x", "z", "c")
BF = jnp.bfloat16
F32 = jnp.float32
SIDE = 4
TOK = 128
BLK = 256
FF = 1024
SLOT = 36
PAIR = 2 * SLOT
PART = SLOT // 2
SHARE = SIDE * PART
SENT = SIDE * PAIR
ROWS = SIDE * SHARE
WIDE = SIDE * BLK


def place(y, x, z, c):
    return ((y * SIDE + x) * SIDE + z) * 2 + c


def groups():
    n = range(SIDE)
    feature, copies, spread = [], [], []
    for k in n:
        for z in n:
            feature.append([place(k, x, z, 0) for x in n])
            feature.append([place(y, k, z, 1) for y in n])
            copies.append([place(y, k, z, 0) for y in n])
            copies.append([place(k, x, z, 1) for x in n])
        spread.append([place(k, x, z, 0) for x in n for z in n])
        spread.append([place(y, k, z, 1) for y in n for z in n])
    return feature, copies, spread


FEATURE, COPIES, SPREAD = groups()


def shifted(value, rings, step):
    pairs = [(g[(i + step) % SIDE], g[i]) for g in rings for i in range(SIDE)]
    return lax.ppermute(value, AXES, pairs)


def grouped(value, rings):
    return lax.all_to_all(value, AXES, 0, 0, axis_index_groups=rings, tiled=True)


def other_core(value):
    return lax.ppermute(value, "c", [(0, 1), (1, 0)])


def iota(shape, dim):
    return lax.broadcasted_iota(jnp.int32, shape, dim)


def dot(a, b):
    return jnp.dot(a, b, preferred_element_type=F32)


def dot_nt(a, b):
    return lax.dot_general(a, b, (((1,), (1,)), ((), ())), preferred_element_type=F32)


def near(value):
    return pltpu.with_memory_space_constraint(value, pltpu.VMEM)


def far(value):
    return pltpu.with_memory_space_constraint(value, pltpu.HBM)


def call(body, outs, args, hbm=(), scratch=(), copies=0, smem=1, limit=20):
    vmem, raw = pl.BlockSpec(memory_space=pltpu.VMEM), pl.BlockSpec(memory_space=pl.ANY)
    specs = [pl.BlockSpec(memory_space=pltpu.SMEM)] * smem
    specs += [raw if isinstance(a, tuple) else vmem for a in args[smem:]]
    held = [pltpu.VMEM(dims, BF) for dims in scratch]
    return pl.pallas_call(
        body,
        out_shape=[(pltpu.HBM if n in hbm else pltpu.VMEM)(dims, BF) for n, dims in enumerate(outs)],
        in_specs=specs,
        out_specs=[raw if n in hbm else vmem for n in range(len(outs))],
        scratch_shapes=held + ([pltpu.SemaphoreType.DMA((copies,))] if copies else []),
        compiler_params=pltpu.CompilerParams(vmem_limit_bytes=limit * 2**20),
    )(*[far(a[0]) if isinstance(a, tuple) else a for a in args])


class Copies:
    def __init__(self, sems):
        self.sems, self.count, self.going = sems, 0, []

    def start(self, src, dst):
        copy = pltpu.make_async_copy(src, dst, self.sems.at[self.count])
        copy.start()
        self.count += 1
        return copy

    def send(self, src, dst):
        self.going.append(self.start(src, dst))

    def drain(self):
        for copy in self.going:
            copy.wait()


def column(kind, near, group, k):
    turned = (near + k) % SIDE
    return jnp.where(kind == 0, turned * SIDE + group, group * SIDE + turned)


def slots(route):
    count = route.shape[0]
    hits = (iota((count, 8), 1) == route).astype(F32)
    earlier = (iota((count, count), 1) < iota((count, count), 0)).astype(BF)
    return jnp.sum(dot(earlier, hits.astype(BF)) * hits, axis=1, keepdims=True).astype(jnp.int32)


def routes_of(*metas):
    return jnp.concatenate([m[:, 0:1] for m in metas], axis=0).astype(F32).astype(jnp.int32)


def pack_body(pos, meta_a, meta_b, tok_b, cot_b, tok_far, cot_far, out_far, tok_a, cot_a, out, sems):
    kind, at = pos[0], pos[1]
    copies = Copies(sems)
    loads = [copies.start(tok_far, tok_a), copies.start(cot_far, cot_a)]
    route = routes_of(meta_a, meta_b)
    target = jnp.where(route % 2 == kind, (route // 2) * PAIR + slots(route), -PAIR)
    rows = iota((2 * TOK, SENT), 1)
    pick_x = jnp.transpose((rows == target).astype(F32)).astype(BF)
    pick_y = jnp.transpose((rows == target + SLOT).astype(F32)).astype(BF)
    weight = jnp.concatenate([meta_a[:, 1:2], meta_b[:, 1:2]], axis=0).astype(F32)
    for load in loads:
        load.wait()
    for d in range(SIDE):
        for k in range(SIDE):
            src = pl.ds(pl.multiple_of(column(kind, at, d, k) * BLK, BLK), BLK)
            x = jnp.concatenate([tok_a[:, src], tok_b[:, src]], axis=0)
            y = jnp.concatenate([cot_a[:, src], cot_b[:, src]], axis=0).astype(F32)
            both = dot(pick_x, x) + dot(pick_y, (y * weight).astype(BF))
            out[d, :, k * BLK : (k + 1) * BLK] = both.astype(BF)
        copies.send(out.at[d], out_far.at[d])
    copies.drain()


def project_body(first, loads, pos, got, *refs):
    if loads:
        given, x, y, parts, kept, sems = refs[:13], refs[13], refs[14], refs[15:19], refs[19:27], refs[27]
        copies = Copies(sems)
        d0, d1, low, high, d3 = given[:5]
        halves = (slice(0, FF // 2), slice(FF // 2, FF))
        going = [copies.start(a, kept[k]) for k, a in ((0, d0), (1, d1), (3, d3))]
        going += [copies.start(a, kept[2].at[rows, :]) for a, rows in zip((low, high), halves)]
        first_up = len(going)
        for t in range(2):
            for k in range(SIDE):
                rows = slice(t * BLK, (t + 1) * BLK)
                going.append(copies.start(given[5 + t * SIDE + k], kept[SIDE + k].at[rows, :]))
    else:
        kept, x, y, parts = refs[:8], refs[8], refs[9], refs[10:14]
    ds, ws = kept[:SIDE], kept[SIDE:]
    q, r = iota((SHARE, SENT), 0), iota((SHARE, SENT), 1)
    home = q + (q // PART) * (PAIR - PART) + first
    for rows, take in ((x, (r == home).astype(BF)), (y, (r == home + SLOT).astype(BF))):
        for k in range(SIDE):
            rows[k * SHARE : (k + 1) * SHARE, :] = dot(take, got[(pos[2] + k) % SIDE]).astype(BF)
    for t in (2, 0, 1):
        if loads and t != 1:
            for copy in going[:first_up] if t == 2 else going[first_up:]:
                copy.wait()
        for n in range(FF // BLK):
            cols = slice(n * BLK, (n + 1) * BLK)
            total = 0.0
            for k in range(SIDE):
                block = slice(k * BLK, (k + 1) * BLK)
                if t == 2:
                    total = total + dot_nt(y[:, block], ds[k][cols, :])
                else:
                    total = total + dot(x[:, block], ws[k][t * BLK : (t + 1) * BLK, cols])
            total = total.astype(BF)
            for k, p in enumerate(parts):
                p[:, t * FF + n * BLK : t * FF + (n + 1) * BLK] = total[k * SHARE : (k + 1) * SHARE]


def activate_body(p0, p1, p2, p3, out):
    for n in range(FF // BLK):
        cols = [slice(t * FF + n * BLK, t * FF + (n + 1) * BLK) for t in range(3)]
        gate, upper, dact = [sum(p[:, c].astype(F32) for p in (p0, p1, p2, p3)) for c in cols]
        sig = jax.nn.sigmoid(gate)
        out[:, cols[0]] = (gate * sig * upper).astype(BF)
        out[:, cols[1]] = (dact * upper * sig * (1.0 + gate * (1.0 - sig))).astype(BF)
        out[:, cols[2]] = (dact * gate * sig).astype(BF)


def turn_body(x_a, x_b, y_a, y_b, two, turned_far, turned, sems):
    copies = Copies(sems)
    for k in (2, 1, 3, 0):
        for n, (a, b) in enumerate(((x_a, x_b), (y_a, y_b))):
            cols = slice(k * BLK, (k + 1) * BLK)
            both = [v[m * SHARE : (m + 1) * SHARE, cols].astype(F32) for m in range(SIDE) for v in (a, b)]
            out = two.at[n] if k == 2 else turned.at[k, n]
            out[...] = jnp.transpose(jnp.concatenate(both, axis=0)).astype(BF)
        if k != 2:
            copies.send(turned.at[k], turned_far.at[k])
    copies.drain()


def block_grads(out, x, y, acts):
    out[0:BLK, :] = dot(x, acts[:, FF : 2 * FF]).astype(BF)
    out[BLK : 2 * BLK, :] = dot(x, acts[:, 2 * FF :]).astype(BF)
    out[2 * BLK :, :] = dot(y, acts[:, 0:FF]).astype(BF)


def first_grads_body(turned, *refs):
    pieces, acts, acts_far, out_far, out, sems = refs[: 2 * SIDE], *refs[2 * SIDE :]
    copies = Copies(sems)
    for n, a in enumerate(pieces):
        at = 2 * (n % SIDE) + n // SIDE
        acts[at * SHARE : (at + 1) * SHARE, :] = a[...]
    copies.send(acts, acts_far)
    block_grads(out, turned[0], turned[1], acts)
    copies.send(out, out_far)
    copies.drain()


def more_grads_body(blocks, turned_far, acts_far, *refs):
    n = len(blocks)
    outs_far, turned, acts, *outs, sems = refs[:n], *refs[n:]
    copies = Copies(sems)
    load = copies.start(acts_far, acts)
    loads = [copies.start(turned_far.at[k], turned.at[i]) for i, k in enumerate(blocks)]
    load.wait()
    for i in range(n):
        loads[i].wait()
        made = outs[0].at[i] if outs else outs_far[i]
        block_grads(made, turned[i, 0], turned[i, 1], acts)
        if outs:
            copies.send(made, outs_far[i])
    copies.drain()


def return_body(pos, acts, *refs):
    weights, back_far, res, slot, back, sems = refs[: 2 * SIDE], *refs[2 * SIDE :]
    copies = Copies(sems)
    for k in range(SIDE):
        d, w, cols = weights[k], weights[SIDE + k], slice(k * BLK, (k + 1) * BLK)
        res[:, cols] = dot(acts[:, 0:FF], d[...]).astype(BF)
        total = dot_nt(acts[:, FF : 2 * FF], w[0:BLK, :]) + dot_nt(acts[:, 2 * FF :], w[BLK:, :])
        slot[:, cols] = total.astype(BF)
    r, q = iota((SENT, 2 * SHARE), 0), iota((SENT, 2 * SHARE), 1)
    step, q = q // SHARE, q % SHARE
    home = q + (q // PART) * (PAIR - PART) + step * PART
    give_m, give_s = (r == home).astype(BF), (r == home + SLOT).astype(BF)
    for k in range(SIDE):
        rows = slice(2 * k * SHARE, 2 * (k + 1) * SHARE)
        back[k] = (dot(give_m, res[rows, :]) + dot(give_s, slot[rows, :])).astype(BF)
        copies.send(back.at[k], back_far.at[(pos[2] + k) % SIDE])
    copies.drain()


def unpack_body(pos, meta_a, meta_b, own, oth, mixed_far, grad_far, mixed, grad, sems):
    kind, at, across = pos[0], pos[1], pos[2]
    copies = Copies(sems)
    rows = iota((TOK, SENT), 1)

    def picks(route, core, mine):
        target = jnp.where(route % 2 == core, (route // 2) * PAIR + slots(route), -PAIR)[mine]
        return (rows == target).astype(BF), (rows == target + SLOT).astype(BF)

    own_m, own_s = picks(routes_of(meta_a, meta_b), kind, slice(0, TOK))
    oth_m, oth_s = picks(routes_of(meta_b, meta_a), 1 - kind, slice(TOK, 2 * TOK))
    weight = meta_a[:, 1:2].astype(F32)
    for b in range(SIDE * SIDE):
        major, minor = b // SIDE, b % SIDE
        own_d = jnp.where(kind == 0, minor, major)
        own_k = (jnp.where(kind == 0, major, minor) - at + SIDE) % SIDE
        oth_d = jnp.where(kind == 0, major, minor)
        oth_k = (jnp.where(kind == 0, minor, major) - across + SIDE) % SIDE
        o = own[own_d, :, pl.ds(pl.multiple_of(own_k * BLK, BLK), BLK)]
        t = oth[oth_d, :, pl.ds(pl.multiple_of(oth_k * BLK, BLK), BLK)]
        cols = slice(b * BLK, (b + 1) * BLK)
        mixed[:, cols] = ((dot(own_m, o) + dot(oth_m, t)) * weight).astype(BF)
        grad[:, cols] = (dot(own_s, o) + dot(oth_s, t)).astype(BF)
        if minor == SIDE - 1:
            done = pl.ds(major * WIDE, WIDE)
            copies.send(mixed.at[:, done], mixed_far.at[:, done])
            copies.send(grad.at[:, done], grad_far.at[:, done])
    copies.drain()


def total_body(n0, n1, n2, n3, gate_far, upper_far, down_far, gate, upper, down, sems):
    copies = Copies(sems)

    def total(t):
        rows = slice(t * BLK, (t + 1) * BLK)
        return sum(n[rows, :].astype(F32) for n in (n0, n1, n2, n3))

    down[...] = jnp.transpose(total(2)).astype(BF)
    copies.send(down, down_far)
    gate[...] = total(0).astype(BF)
    copies.send(gate, gate_far)
    upper[...] = total(1).astype(BF)
    copies.send(upper, upper_far)
    copies.drain()


def exchanged(value):
    rows = value.reshape(SIDE * SIDE, PAIR, WIDE)
    return near(grouped(rows, SPREAD).reshape(SIDE, SENT, WIDE))


def layer(tokens, probs, routes, w_gate, w_up, w_down, cotangent):
    y, x, c = lax.axis_index("y"), lax.axis_index("x"), lax.axis_index("c")
    pos = jnp.stack([c, jnp.where(c == 0, y, x), jnp.where(c == 0, x, y)]).astype(jnp.int32)
    meta = jnp.concatenate([routes.astype(BF), probs], axis=1)
    meta_b, tok_b, cot_b = other_core(meta), other_core(tokens), other_core(cotangent)
    d0, g0, u0 = w_down[0], w_gate[0], w_up[0]
    g1, g3 = shifted(g0, COPIES, 1), shifted(g0, COPIES, -1)
    u1, u3 = shifted(u0, COPIES, 1), shifted(u0, COPIES, -1)
    d1, d3 = shifted(d0, COPIES, 1), shifted(d0, COPIES, -1)
    half = FF // 2
    g2 = (shifted(g3, COPIES, -1))
    u2 = (shifted(u1, COPIES, 1))
    low, high = (shifted(d1[:half], COPIES, 1)), (shifted(d3[half:], COPIES, -1))
    weights = [(d0,), (d1,), (low,), (high,), (d3,), (g0,), (g1,), (g2,), (g3,), (u0,), (u1,), (u2,), (u3,)]
    (sent,) = call(
        pack_body,
        [(SIDE, SENT, WIDE)],
        [pos, meta, meta_b, near(tok_b), near(cot_b), (tokens,), (cotangent,)],
        hbm=(0,),
        scratch=[tokens.shape, tokens.shape, (SIDE, SENT, WIDE)],
        copies=2 + SIDE,
    )
    got = exchanged(sent)
    xs, ys, parts, pieces = [], [], [], []
    kept = weights
    for p in (0, 1):
        x, y, *part = call(
            functools.partial(project_body, p * PART, p == 0),
            [(ROWS, WIDE)] * 2 + [(SHARE, 3 * FF)] * SIDE + ([] if p else [(FF, BLK)] * SIDE + [(2 * BLK, FF)] * SIDE),
            [pos, got, *kept],
            copies=0 if p else len(weights),
        )
        if p == 0:
            part, kept = part[:SIDE], part[SIDE:]
        parts.append([part[0]] + [near(shifted(part[k], FEATURE, -k)) for k in (1, 2, 3)])
        xs.append(x)
        ys.append(y)
    for p in (0, 1):
        (act,) = call(activate_body, [(SHARE, 3 * FF)], parts[p], smem=0)
        pieces += [act] + [near(shifted(act, FEATURE, k)) for k in (1, 2, -1)]
    pair = (2, BLK, 2 * ROWS)
    block = (3 * BLK, FF)
    whole = (2 * ROWS, 3 * FF)
    two, turned = call(
        turn_body, [pair, (SIDE, *pair)], [*xs, *ys], smem=0, hbm=(1,), scratch=[(SIDE, *pair)], copies=3
    )
    acts, acts_far, n2 = call(
        first_grads_body, [whole, whole, block], [two, *pieces], smem=0, hbm=(1, 2), scratch=[block], copies=2
    )
    n2 = near(shifted(n2, COPIES, -2))
    (back,) = call(
        return_body,
        [(SIDE, SENT, WIDE)],
        [pos, near(acts), *kept],
        hbm=(0,),
        scratch=[(2 * ROWS, WIDE)] * 2 + [(SIDE, SENT, WIDE)],
        copies=SIDE,
    )
    own = exchanged(back)
    ns = {}
    for blocks in ((1, 3), (0,)):
        many = len(blocks)
        done = call(
            functools.partial(more_grads_body, blocks),
            [block] * many,
            [(turned,), (acts_far,)],
            smem=0,
            hbm=tuple(range(many)) if many > 1 else (),
            scratch=[(many, *pair), whole] + [(many, *block)] * (many > 1),
            copies=1 + 2 * many,
        )
        ns.update(zip(blocks, done))
    n1, n3 = near(shifted(ns[1], COPIES, -1)), near(shifted(ns[3], COPIES, 1))
    oth = near(other_core(own))
    mixed, into = call(
        unpack_body,
        [tokens.shape] * 2,
        [pos, meta, meta_b, own, oth],
        hbm=(0, 1),
        scratch=[tokens.shape] * 2,
        copies=2 * SIDE,
    )
    shapes = [(BLK, FF), (BLK, FF), (FF, BLK)]
    gate, upper, down = call(total_body, shapes, [ns[0], n1, n2, n3], smem=0, hbm=(0, 1, 2), scratch=shapes, copies=3)
    return mixed, into, gate[None], upper[None], down[None]


def solution(mesh):
    finer = Mesh(mesh.devices.reshape(SIDE, SIDE, SIDE, 2), AXES)
    rows = P(AXES, None)
    wide = P(("z", "c"), ("y", "x"), None)
    tall = P(("z", "c"), None, ("y", "x"))
    return jax.shard_map(
        layer,
        mesh=finer,
        in_specs=(rows, rows, rows, wide, wide, tall, rows),
        out_specs=(rows, rows, wide, wide, tall),
        check_vma=False,
    )
```

```python
import functools

import jax
import jax.numpy as jnp
from jax import lax
from jax.experimental import pallas as pl
from jax.experimental.pallas import tpu as pltpu
from jax.sharding import Mesh
from jax.sharding import PartitionSpec as P


AXES = ("y", "x", "z", "c")
BF = jnp.bfloat16
F32 = jnp.float32
SIDE = 4
TOK = 128
BLK = 256
FF = 1024
SLOT = 36
PAIR = 2 * SLOT
PART = SLOT // 2
SHARE = SIDE * PART
SENT = SIDE * PAIR
ROWS = SIDE * SHARE
WIDE = SIDE * BLK


def place(y, x, z, c):
    return ((y * SIDE + x) * SIDE + z) * 2 + c


def groups():
    n = range(SIDE)
    feature, copies, spread = [], [], []
    for k in n:
        for z in n:
            feature.append([place(k, x, z, 0) for x in n])
            feature.append([place(y, k, z, 1) for y in n])
            copies.append([place(y, k, z, 0) for y in n])
            copies.append([place(k, x, z, 1) for x in n])
        spread.append([place(k, x, z, 0) for x in n for z in n])
        spread.append([place(y, k, z, 1) for y in n for z in n])
    return feature, copies, spread


FEATURE, COPIES, SPREAD = groups()


def shifted(value, rings, step):
    pairs = [(g[(i + step) % SIDE], g[i]) for g in rings for i in range(SIDE)]
    return lax.ppermute(value, AXES, pairs)


def grouped(value, rings):
    return lax.all_to_all(value, AXES, 0, 0, axis_index_groups=rings, tiled=True)


def other_core(value):
    return lax.ppermute(value, "c", [(0, 1), (1, 0)])


def iota(shape, dim):
    return lax.broadcasted_iota(jnp.int32, shape, dim)


def dot(a, b):
    return jnp.dot(a, b, preferred_element_type=F32)


def dot_nt(a, b):
    return lax.dot_general(a, b, (((1,), (1,)), ((), ())), preferred_element_type=F32)


def near(value):
    return pltpu.with_memory_space_constraint(value, pltpu.VMEM)


def far(value):
    return pltpu.with_memory_space_constraint(value, pltpu.HBM)


def call(body, outs, args, hbm=(), scratch=(), copies=0, smem=1, limit=20):
    vmem, raw = pl.BlockSpec(memory_space=pltpu.VMEM), pl.BlockSpec(memory_space=pl.ANY)
    specs = [pl.BlockSpec(memory_space=pltpu.SMEM)] * smem
    specs += [raw if isinstance(a, tuple) else vmem for a in args[smem:]]
    held = [pltpu.VMEM(dims, BF) for dims in scratch]
    return pl.pallas_call(
        body,
        out_shape=[(pltpu.HBM if n in hbm else pltpu.VMEM)(dims, BF) for n, dims in enumerate(outs)],
        in_specs=specs,
        out_specs=[raw if n in hbm else vmem for n in range(len(outs))],
        scratch_shapes=held + ([pltpu.SemaphoreType.DMA((copies,))] if copies else []),
        compiler_params=pltpu.CompilerParams(vmem_limit_bytes=limit * 2**20),
    )(*[far(a[0]) if isinstance(a, tuple) else a for a in args])


class Copies:
    def __init__(self, sems):
        self.sems, self.count, self.going = sems, 0, []

    def start(self, src, dst):
        copy = pltpu.make_async_copy(src, dst, self.sems.at[self.count])
        copy.start()
        self.count += 1
        return copy

    def send(self, src, dst):
        self.going.append(self.start(src, dst))

    def drain(self):
        for copy in self.going:
            copy.wait()


def column(kind, near, group, k):
    turned = (near + k) % SIDE
    return jnp.where(kind == 0, turned * SIDE + group, group * SIDE + turned)


def slots(route):
    count = route.shape[0]
    hits = (iota((count, 8), 1) == route).astype(F32)
    earlier = (iota((count, count), 1) < iota((count, count), 0)).astype(BF)
    return jnp.sum(dot(earlier, hits.astype(BF)) * hits, axis=1, keepdims=True).astype(jnp.int32)


def routes_of(*metas):
    return jnp.concatenate([m[:, 0:1] for m in metas], axis=0).astype(F32).astype(jnp.int32)


def pack_body(pos, meta_a, meta_b, tok_b, cot_b, tok_far, cot_far, out_far, tok_a, cot_a, out, sems):
    kind, at = pos[0], pos[1]
    copies = Copies(sems)
    loads = [copies.start(tok_far, tok_a), copies.start(cot_far, cot_a)]
    route = routes_of(meta_a, meta_b)
    target = jnp.where(route % 2 == kind, (route // 2) * PAIR + slots(route), -PAIR)
    rows = iota((2 * TOK, SENT), 1)
    pick_x = jnp.transpose((rows == target).astype(F32)).astype(BF)
    pick_y = jnp.transpose((rows == target + SLOT).astype(F32)).astype(BF)
    weight = jnp.concatenate([meta_a[:, 1:2], meta_b[:, 1:2]], axis=0).astype(F32)
    for load in loads:
        load.wait()
    for d in range(SIDE):
        for k in range(SIDE):
            src = pl.ds(pl.multiple_of(column(kind, at, d, k) * BLK, BLK), BLK)
            x = jnp.concatenate([tok_a[:, src], tok_b[:, src]], axis=0)
            y = jnp.concatenate([cot_a[:, src], cot_b[:, src]], axis=0).astype(F32)
            both = dot(pick_x, x) + dot(pick_y, (y * weight).astype(BF))
            out[d, :, k * BLK : (k + 1) * BLK] = both.astype(BF)
        copies.send(out.at[d], out_far.at[d])
    copies.drain()


def project_body(first, loads, pos, got, *refs):
    if loads:
        given, x, y, parts, kept, sems = refs[:13], refs[13], refs[14], refs[15:19], refs[19:27], refs[27]
        copies = Copies(sems)
        d0, d1, low, high, d3 = given[:5]
        halves = (slice(0, FF // 2), slice(FF // 2, FF))
        going = [copies.start(a, kept[k]) for k, a in ((0, d0), (1, d1), (3, d3))]
        going += [copies.start(a, kept[2].at[rows, :]) for a, rows in zip((low, high), halves)]
        first_up = len(going)
        for t in range(2):
            for k in range(SIDE):
                rows = slice(t * BLK, (t + 1) * BLK)
                going.append(copies.start(given[5 + t * SIDE + k], kept[SIDE + k].at[rows, :]))
    else:
        kept, x, y, parts = refs[:8], refs[8], refs[9], refs[10:14]
    ds, ws = kept[:SIDE], kept[SIDE:]
    q, r = iota((2 * SHARE, SENT), 0), iota((2 * SHARE, SENT), 1)
    kind, q = q // SHARE, q % SHARE
    take = (r == q + (q // PART) * (PAIR - PART) + first + kind * SLOT).astype(BF)
    for k in range(SIDE):
        both = dot(take, got[(pos[2] + k) % SIDE]).astype(BF)
        x[k * SHARE : (k + 1) * SHARE, :] = both[0:SHARE]
        y[k * SHARE : (k + 1) * SHARE, :] = both[SHARE:]
    for t in (2, 0, 1):
        if loads:
            ends = (first_up, first_up + SIDE, first_up + 2 * SIDE)
            for copy in going[0:first_up] if t == 2 else going[ends[t] : ends[t + 1]]:
                copy.wait()
        for n in range(FF // BLK):
            cols = slice(n * BLK, (n + 1) * BLK)
            total = 0.0
            for k in range(SIDE):
                block = slice(k * BLK, (k + 1) * BLK)
                if t == 2:
                    total = total + dot_nt(y[:, block], ds[k][cols, :])
                else:
                    total = total + dot(x[:, block], ws[k][t * BLK : (t + 1) * BLK, cols])
            total = total.astype(BF)
            for k, p in enumerate(parts):
                p[:, t * FF + n * BLK : t * FF + (n + 1) * BLK] = total[k * SHARE : (k + 1) * SHARE]


def activate_body(p0, p1, p2, p3, out):
    for n in range(FF // BLK):
        cols = [slice(t * FF + n * BLK, t * FF + (n + 1) * BLK) for t in range(3)]
        gate, upper, dact = [sum(p[:, c].astype(F32) for p in (p0, p1, p2, p3)) for c in cols]
        sig = jax.nn.sigmoid(gate)
        out[:, cols[0]] = (gate * sig * upper).astype(BF)
        out[:, cols[1]] = (dact * upper * sig * (1.0 + gate * (1.0 - sig))).astype(BF)
        out[:, cols[2]] = (dact * gate * sig).astype(BF)


def turn_body(x_a, x_b, y_a, y_b, two, turned_far, turned, sems):
    copies = Copies(sems)
    for k in (2, 1, 3, 0):
        for n, (a, b) in enumerate(((x_a, x_b), (y_a, y_b))):
            cols = slice(k * BLK, (k + 1) * BLK)
            both = [v[m * SHARE : (m + 1) * SHARE, cols].astype(F32) for m in range(SIDE) for v in (a, b)]
            out = two.at[n] if k == 2 else turned.at[k, n]
            out[...] = jnp.transpose(jnp.concatenate(both, axis=0)).astype(BF)
        if k != 2:
            copies.send(turned.at[k], turned_far.at[k])
    copies.drain()


def block_grads(out, x, y, acts):
    out[0:BLK, :] = dot(x, acts[:, FF : 2 * FF]).astype(BF)
    out[BLK : 2 * BLK, :] = dot(x, acts[:, 2 * FF :]).astype(BF)
    out[2 * BLK :, :] = dot(y, acts[:, 0:FF]).astype(BF)


def first_grads_body(turned, *refs):
    pieces, acts, acts_far, out_far, out, sems = refs[: 2 * SIDE], *refs[2 * SIDE :]
    copies = Copies(sems)
    for n, a in enumerate(pieces):
        at = 2 * (n % SIDE) + n // SIDE
        acts[at * SHARE : (at + 1) * SHARE, :] = a[...]
    copies.send(acts, acts_far)
    block_grads(out, turned[0], turned[1], acts)
    copies.send(out, out_far)
    copies.drain()


def more_grads_body(blocks, turned_far, acts_far, *refs):
    n = len(blocks)
    outs_far, turned, acts, *outs, sems = refs[:n], *refs[n:]
    copies = Copies(sems)
    load = copies.start(acts_far, acts)
    loads = [copies.start(turned_far.at[k], turned.at[i]) for i, k in enumerate(blocks)]
    load.wait()
    for i in range(n):
        loads[i].wait()
        made = outs[0].at[i] if outs else outs_far[i]
        block_grads(made, turned[i, 0], turned[i, 1], acts)
        if outs:
            copies.send(made, outs_far[i])
    copies.drain()


def return_body(pos, acts, *refs):
    weights, back_far, res, slot, back, sems = refs[: 2 * SIDE], *refs[2 * SIDE :]
    copies = Copies(sems)
    for k in range(SIDE):
        d, w, cols = weights[k], weights[SIDE + k], slice(k * BLK, (k + 1) * BLK)
        res[:, cols] = dot(acts[:, 0:FF], d[...]).astype(BF)
        total = dot_nt(acts[:, FF : 2 * FF], w[0:BLK, :]) + dot_nt(acts[:, 2 * FF :], w[BLK:, :])
        slot[:, cols] = total.astype(BF)
    r, q = iota((SENT, 2 * SHARE), 0), iota((SENT, 2 * SHARE), 1)
    step, q = q // SHARE, q % SHARE
    home = q + (q // PART) * (PAIR - PART) + step * PART
    give_m, give_s = (r == home).astype(BF), (r == home + SLOT).astype(BF)
    for k in range(SIDE):
        rows = slice(2 * k * SHARE, 2 * (k + 1) * SHARE)
        back[k] = (dot(give_m, res[rows, :]) + dot(give_s, slot[rows, :])).astype(BF)
        copies.send(back.at[k], back_far.at[(pos[2] + k) % SIDE])
    copies.drain()


def unpack_body(pos, meta_a, meta_b, own, oth, mixed_far, grad_far, mixed, grad, sems):
    kind, at, across = pos[0], pos[1], pos[2]
    copies = Copies(sems)
    rows = iota((TOK, SENT), 1)

    def picks(route, core, mine):
        target = jnp.where(route % 2 == core, (route // 2) * PAIR + slots(route), -PAIR)[mine]
        return jnp.concatenate([(rows == target).astype(BF), (rows == target + SLOT).astype(BF)], axis=0)

    own_both = picks(routes_of(meta_a, meta_b), kind, slice(0, TOK))
    oth_both = picks(routes_of(meta_b, meta_a), 1 - kind, slice(TOK, 2 * TOK))
    weight = meta_a[:, 1:2].astype(F32)
    for b in range(SIDE * SIDE):
        major, minor = b // SIDE, b % SIDE
        own_d = jnp.where(kind == 0, minor, major)
        own_k = (jnp.where(kind == 0, major, minor) - at + SIDE) % SIDE
        oth_d = jnp.where(kind == 0, major, minor)
        oth_k = (jnp.where(kind == 0, minor, major) - across + SIDE) % SIDE
        o = own[own_d, :, pl.ds(pl.multiple_of(own_k * BLK, BLK), BLK)]
        t = oth[oth_d, :, pl.ds(pl.multiple_of(oth_k * BLK, BLK), BLK)]
        cols = slice(b * BLK, (b + 1) * BLK)
        both = dot(own_both, o) + dot(oth_both, t)
        mixed[:, cols] = (both[0:TOK] * weight).astype(BF)
        grad[:, cols] = both[TOK:].astype(BF)
        if minor == SIDE - 1:
            done = pl.ds(major * WIDE, WIDE)
            copies.send(mixed.at[:, done], mixed_far.at[:, done])
            copies.send(grad.at[:, done], grad_far.at[:, done])
    copies.drain()


def total_body(n0, n1, n2, n3, gate_far, upper_far, down_far, gate, upper, down, sems):
    copies = Copies(sems)

    def total(t):
        rows = slice(t * BLK, (t + 1) * BLK)
        return sum(n[rows, :].astype(F32) for n in (n0, n1, n2, n3))

    down[...] = jnp.transpose(total(2)).astype(BF)
    copies.send(down, down_far)
    gate[...] = total(0).astype(BF)
    copies.send(gate, gate_far)
    upper[...] = total(1).astype(BF)
    copies.send(upper, upper_far)
    copies.drain()


def exchanged(value):
    rows = value.reshape(SIDE * SIDE, PAIR, WIDE)
    return near(grouped(rows, SPREAD).reshape(SIDE, SENT, WIDE))


def layer(tokens, probs, routes, w_gate, w_up, w_down, cotangent):
    y, x, c = lax.axis_index("y"), lax.axis_index("x"), lax.axis_index("c")
    pos = jnp.stack([c, jnp.where(c == 0, y, x), jnp.where(c == 0, x, y)]).astype(jnp.int32)
    meta = jnp.concatenate([routes.astype(BF), probs], axis=1)
    meta_b, tok_b, cot_b = other_core(meta), other_core(tokens), other_core(cotangent)
    d0, g0, u0 = w_down[0], w_gate[0], w_up[0]
    g1, g3 = shifted(g0, COPIES, 1), shifted(g0, COPIES, -1)
    u1, u3 = shifted(u0, COPIES, 1), shifted(u0, COPIES, -1)
    d1, d3 = shifted(d0, COPIES, 1), shifted(d0, COPIES, -1)
    half = FF // 2
    g2 = (shifted(g3, COPIES, -1))
    u2 = (shifted(u1, COPIES, 1))
    low, high = (shifted(d1[:half], COPIES, 1)), (shifted(d3[half:], COPIES, -1))
    weights = [(d0,), (d1,), (low,), (high,), (d3,), (g0,), (g1,), (g2,), (g3,), (u0,), (u1,), (u2,), (u3,)]
    (sent,) = call(
        pack_body,
        [(SIDE, SENT, WIDE)],
        [pos, meta, meta_b, near(tok_b), near(cot_b), (tokens,), (cotangent,)],
        hbm=(0,),
        scratch=[tokens.shape, tokens.shape, (SIDE, SENT, WIDE)],
        copies=2 + SIDE,
    )
    got = exchanged(sent)
    xs, ys, parts, pieces = [], [], [], []
    kept = weights
    for p in (0, 1):
        x, y, *part = call(
            functools.partial(project_body, p * PART, p == 0),
            [(ROWS, WIDE)] * 2 + [(SHARE, 3 * FF)] * SIDE + ([] if p else [(FF, BLK)] * SIDE + [(2 * BLK, FF)] * SIDE),
            [pos, got, *kept],
            copies=0 if p else len(weights),
        )
        if p == 0:
            part, kept = part[:SIDE], part[SIDE:]
        parts.append([part[0]] + [near(shifted(part[k], FEATURE, -k)) for k in (1, 2, 3)])
        xs.append(x)
        ys.append(y)
    for p in (0, 1):
        (act,) = call(activate_body, [(SHARE, 3 * FF)], parts[p], smem=0)
        pieces += [act] + [near(shifted(act, FEATURE, k)) for k in (1, 2, -1)]
    pair = (2, BLK, 2 * ROWS)
    block = (3 * BLK, FF)
    whole = (2 * ROWS, 3 * FF)
    two, turned = call(
        turn_body, [pair, (SIDE, *pair)], [*xs, *ys], smem=0, hbm=(1,), scratch=[(SIDE, *pair)], copies=3
    )
    acts, acts_far, n2 = call(
        first_grads_body, [whole, whole, block], [two, *pieces], smem=0, hbm=(1, 2), scratch=[block], copies=2
    )
    n2 = near(shifted(n2, COPIES, -2))
    (back,) = call(
        return_body,
        [(SIDE, SENT, WIDE)],
        [pos, near(acts), *kept],
        hbm=(0,),
        scratch=[(2 * ROWS, WIDE)] * 2 + [(SIDE, SENT, WIDE)],
        copies=SIDE,
    )
    own = exchanged(back)
    ns = {}
    for blocks in ((1, 3), (0,)):
        many = len(blocks)
        done = call(
            functools.partial(more_grads_body, blocks),
            [block] * many,
            [(turned,), (acts_far,)],
            smem=0,
            hbm=tuple(range(many)) if many > 1 else (),
            scratch=[(many, *pair), whole] + [(many, *block)] * (many > 1),
            copies=1 + 2 * many,
        )
        ns.update(zip(blocks, done))
    n1, n3 = near(shifted(ns[1], COPIES, -1)), near(shifted(ns[3], COPIES, 1))
    oth = near(other_core(own))
    mixed, into = call(
        unpack_body,
        [tokens.shape] * 2,
        [pos, meta, meta_b, own, oth],
        hbm=(0, 1),
        scratch=[tokens.shape] * 2,
        copies=2 * SIDE,
    )
    shapes = [(BLK, FF), (BLK, FF), (FF, BLK)]
    gate, upper, down = call(total_body, shapes, [ns[0], n1, n2, n3], smem=0, hbm=(0, 1, 2), scratch=shapes, copies=3)
    return mixed, into, gate[None], upper[None], down[None]


def solution(mesh):
    finer = Mesh(mesh.devices.reshape(SIDE, SIDE, SIDE, 2), AXES)
    rows = P(AXES, None)
    wide = P(("z", "c"), ("y", "x"), None)
    tall = P(("z", "c"), None, ("y", "x"))
    return jax.shard_map(
        layer,
        mesh=finer,
        in_specs=(rows, rows, rows, wide, wide, tall, rows),
        out_specs=(rows, rows, wide, wide, tall),
        check_vma=False,
    )
```
